128 devices in a mesh: energy: 32 (over y, x, core), mom: 4 (over z).
Axes of the slice: x: 4, y: 4, z: 4, core: 2. Of those that a mesh axis runs over, the one named last changes fastest.
Arguments:
- lesser: float32 [4, 32, 4, 4, 2, 128, 128], P(None, 'energy', 'mom'), as said below
- greater: float32 [4, 32, 4, 4, 2, 128, 128], P(None, 'energy', 'mom'), as said below
- hamiltonian: float32 [4, 4, 2, 128, 128], P('mom'), as said below
- coupling: float32 [4, 2, 128, 128], P('mom'), may hold values from -0.25 to 0.25
- shift: int32 [1], replicated, may hold values from 1 to 7
- phonon_weight: float32 [2], replicated, may hold values from 0.1 to 0.5
Outputs:
- lesser_next: float32 [4, 32, 4, 4, 2, 128, 128], P(None, 'energy', 'mom')
- greater_next: float32 [4, 32, 4, 4, 2, 128, 128], P(None, 'energy', 'mom')
- current: float32 [], replicated
The draws below stay inside these ranges and needn't reach their ends.
Inputs may be any that keep to these rules, and one draw needn't show every extreme that they name: `lesser`: in each block the complex matrix is i times a Hermitian positive definite matrix. `greater`: in each block the complex matrix is -i times a Hermitian positive definite matrix. `hamiltonian`: each block is Hermitian: real part symmetric, imaginary part antisymmetric.
All inputs are finite; a program needn't handle non-finite values.
Results may differ from the reference program's by a relative error of at most 0.0001.
Values sent between devices are 32-bit elements; how exact they have to be, the bound alone decides.
A program may use at most 128 MiB of HBM per device.

```python
import math
import jax
import jax.numpy as jnp
from jax import lax

B = 128
S = 4
E_DEV = 4
SMAX = 7
NE = 128
NK = 4
N_ENERGY = 32


def occupied(key, sign):
    parts = jax.random.split(key, 3)
    leading = (E_DEV, NE // E_DEV, NK, S)
    real = jax.random.normal(parts[0], leading + (B, B), jnp.float32)
    imag = jax.random.normal(parts[1], leading + (B, B), jnp.float32)
    scale = 1.0 / (2.0 * B)
    herm_re = (jnp.einsum('...ij,...kj->...ik', real, real, precision=lax.Precision.HIGHEST) + jnp.einsum('...ij,...kj->...ik', imag, imag, precision=lax.Precision.HIGHEST)) * scale
    herm_im = (jnp.einsum('...ij,...kj->...ik', imag, real, precision=lax.Precision.HIGHEST) - jnp.einsum('...ij,...kj->...ik', real, imag, precision=lax.Precision.HIGHEST)) * scale
    diagonal = jax.random.uniform(parts[2], leading + (B,), jnp.float32, 0.2, 1.0)
    herm_re = herm_re + diagonal[..., None] * jnp.eye(B, dtype=jnp.float32)
    return jnp.stack([-sign * herm_im, sign * herm_re], 4)


def draw_lesser(key, part):
    return occupied(jax.random.fold_in(key, 11), 1.0)


def draw_greater(key, part):
    return occupied(jax.random.fold_in(key, 12), -1.0)


def draw_hamiltonian(key, part):
    parts = jax.random.split(jax.random.fold_in(key, 13), 3)
    shape = (NK, S, B, B)
    spread = 0.5 / B ** 0.5
    real = jax.random.normal(parts[0], shape, jnp.float32) * spread
    imag = jax.random.normal(parts[1], shape, jnp.float32) * spread
    onsite = jax.random.uniform(parts[2], (NK, S, B), jnp.float32, -1.0, 1.0)
    real = real + jnp.swapaxes(real, -1, -2) + onsite[..., None] * jnp.eye(B, dtype=jnp.float32)
    imag = imag - jnp.swapaxes(imag, -1, -2)
    return jnp.stack([real, imag], 2)


def shard_levels(rng, shape, shards, least, largest):
    gain = 1.0
    for dim, blocks in shards:
        draws = jax.random.uniform(jax.random.fold_in(jax.random.fold_in(rng, 6), dim), (blocks,), jnp.float32, least / len(shards), largest / len(shards))
        gain = gain * jnp.repeat(jnp.exp(draws), shape[dim] // blocks).reshape((-1,) + (1,) * (len(shape) - 1 - dim))
    return gain


def noise(own_key, shape, scale, bound, shards=(), held_as=jnp.bfloat16):
    loudness = shard_levels(own_key, shape, shards, -0.22, 0.18) if shards else 1.0
    values = jax.random.normal(own_key, shape, jnp.float32) * scale * loudness
    return jnp.minimum(jnp.maximum(values, -bound), bound).astype(held_as)


def setup_inputs(seed: int = 0) -> dict:
    key_list = jax.random.split(jax.random.key(seed), 7)
    return {
        "lesser": draw_lesser(jax.random.fold_in(key_list[6], 71), 0),
        "greater": draw_greater(jax.random.fold_in(key_list[6], 71), 0),
        "hamiltonian": draw_hamiltonian(jax.random.fold_in(key_list[6], 71), 0),
        "coupling": noise(key_list[3], (NK, 2, B, B), (4 * B) ** -0.5, 0.25, ((0, 4),), jnp.float32),
        "shift": jax.random.randint(key_list[4], (1,), 1, SMAX + 1).astype(jnp.int32),
        "phonon_weight": jnp.clip(jnp.exp(jax.random.uniform(key_list[5], (2,), jnp.float32, math.log(0.1), math.log(0.5))), 0.1, 0.5),
    }


broaden = 0.2
contact_rate = 0.5
left_level = 0.3
right_level = -0.3
thermal = 0.1
band_edge = 2.0
precise = lax.Precision.HIGHEST

def product(left, right):
    return jnp.einsum('...ij,...jk->...ik', left, right, precision=precise)

def cmul(left, right):
    return (product(left[0], right[0]) - product(left[1], right[1]), product(left[0], right[1]) + product(left[1], right[0]))

def dagger(value):
    return (jnp.swapaxes(value[0], -1, -2), -jnp.swapaxes(value[1], -1, -2))

def sandwich(outer, inner):
    return cmul(cmul(outer, inner), dagger(outer))

def invert(matrix):
    real, imag = matrix
    width = real.shape[-1]
    kernel = jnp.concatenate([jnp.concatenate([real, -imag], -1), jnp.concatenate([imag, real], -1)], -2)
    normal = product(jnp.swapaxes(kernel, -1, -2), kernel)
    lower = jnp.linalg.cholesky(normal)
    rhs = jnp.concatenate([jnp.swapaxes(real, -1, -2), -jnp.swapaxes(imag, -1, -2)], -2)
    middle = jax.scipy.linalg.solve_triangular(lower, rhs, lower=True)
    result = jax.scipy.linalg.solve_triangular(lower, middle, lower=True, trans=1)
    guess = (result[..., :width, :], result[..., width:, :])
    check = cmul(matrix, guess)
    eye = jnp.eye(width, dtype=jnp.float32)
    return cmul(guess, (2.0 * eye - check[0], -check[1]))

def transport(energy, hamiltonian, coupling, sig_less, sig_great):
    slabs = hamiltonian.shape[1]
    width = hamiltonian.shape[-1]
    eye = jnp.eye(width, dtype=jnp.float32)
    level = energy[:, None, None]
    hop = (coupling[:, 0], coupling[:, 1])
    hop_back = dagger(hop)
    fill_left = jax.nn.sigmoid((left_level - energy) / thermal)
    fill_right = jax.nn.sigmoid((right_level - energy) / thermal)
    forward_r = []
    forward_l = []
    for slab in range(slabs):
        less_re = sig_less[:, slab, 0]
        less_im = sig_less[:, slab, 1]
        system_re = level * eye - hamiltonian[:, slab, 0] - 0.5 * (sig_great[:, slab, 0] - less_re)
        system_im = broaden * eye - hamiltonian[:, slab, 1] - 0.5 * (sig_great[:, slab, 1] - less_im)
        inject_re = less_re
        inject_im = less_im
        if slab == 0 or slab == slabs - 1:
            filling = fill_left if slab == 0 else fill_right
            system_im = system_im + contact_rate * eye
            inject_im = inject_im + 2.0 * contact_rate * filling[:, None, None] * eye
        if slab > 0:
            folded = sandwich(hop, forward_r[-1])
            system_re = system_re - folded[0]
            system_im = system_im - folded[1]
            carried = sandwich(hop, forward_l[-1])
            inject_re = inject_re + carried[0]
            inject_im = inject_im + carried[1]
        green = invert((system_re, system_im))
        forward_r.append(green)
        forward_l.append(sandwich(green, (inject_re, inject_im)))
    full_r = forward_r[-1]
    full_l = forward_l[-1]
    outs_r = [full_r]
    outs_l = [full_l]
    for slab in range(slabs - 2, -1, -1):
        green = forward_r[slab]
        green_l = forward_l[slab]
        lead = cmul(green, hop_back)
        spread = cmul(lead, full_r)
        tail = cmul(hop, green)
        extra = cmul(spread, tail)
        new_r = (green[0] + extra[0], green[1] + extra[1])
        cross = cmul(spread, cmul(hop, green_l))
        inner = sandwich(lead, full_l)
        cross_d = dagger(cross)
        new_l = (green_l[0] + inner[0] + cross[0] - cross_d[0], green_l[1] + inner[1] + cross[1] - cross_d[1])
        full_r = new_r
        full_l = new_l
        outs_r.insert(0, full_r)
        outs_l.insert(0, full_l)
    less_blocks = jnp.stack([jnp.stack([value[0], value[1]], 1) for value in outs_l], 1)
    great_blocks = jnp.stack([jnp.stack([outs_l[k][0] + outs_r[k][0] - jnp.swapaxes(outs_r[k][0], -1, -2), outs_l[k][1] + outs_r[k][1] + jnp.swapaxes(outs_r[k][1], -1, -2)], 1) for k in range(slabs)], 1)
    great_trace = jnp.trace(great_blocks[:, 0, 1], axis1=-2, axis2=-1)
    less_trace = jnp.trace(less_blocks[:, 0, 1], axis1=-2, axis2=-1)
    flowing = -(2.0 * contact_rate * fill_left * great_trace + 2.0 * contact_rate * (1.0 - fill_left) * less_trace)
    return (less_blocks, great_blocks, flowing)

def reference(lesser, greater, hamiltonian, coupling, shift, phonon_weight):
    total = E_DEV * N_ENERGY
    tail_shape = (S, 2, B, B)
    mean_less = (jnp.sum(lesser, axis=2) / NK).reshape((total,) + tail_shape)
    mean_great = (jnp.sum(greater, axis=2) / NK).reshape((total,) + tail_shape)
    amount = shift[0].astype(jnp.int32)
    blank = jnp.zeros((SMAX,) + tail_shape, jnp.float32)

    def moved(field, offset):
        padded = jnp.concatenate([blank, field, blank], 0)
        return lax.dynamic_slice_in_dim(padded, (SMAX + offset).astype(jnp.int32), total, 0)
    emission = phonon_weight[0]
    absorption = phonon_weight[1]
    sig_less = emission * moved(mean_less, amount) + absorption * moved(mean_less, -amount)
    sig_great = emission * moved(mean_great, -amount) + absorption * moved(mean_great, amount)
    grid = (jnp.arange(total).astype(jnp.float32) + 0.5) * (2.0 * band_edge / total) - band_edge

    def solve_one(items):
        energy, one_less, one_great = items
        energies = jnp.broadcast_to(energy, (NK,))
        less_wide = jnp.broadcast_to(one_less, (NK,) + tail_shape)
        great_wide = jnp.broadcast_to(one_great, (NK,) + tail_shape)
        return transport(energies, hamiltonian, coupling, less_wide, great_wide)
    less_new, great_new, flowing = lax.map(solve_one, (grid, sig_less, sig_great))
    full_shape = (E_DEV, N_ENERGY, NK) + tail_shape
    current = jnp.sum(flowing) * (2.0 * band_edge / total)
    return (less_new.reshape(full_shape), great_new.reshape(full_shape), current)
```

```python
import functools

import jax
import jax.numpy as jnp
from jax import lax
from jax.experimental import pallas as pl
from jax.experimental.pallas import tpu as pltpu
from jax.sharding import PartitionSpec as P

SMAX = 7
broaden = 0.2
contact_rate = 0.5
left_level = 0.3
right_level = -0.3
thermal = 0.1
band_edge = 2.0

W = 128
BF = jnp.bfloat16
F32 = jnp.float32
LEAST = 0.03


def store(ref, real, imag):
    for row, part in ((0, real), (W, imag)):
        high = part.astype(BF)
        ref[row : row + W, :W] = high
        ref[row : row + W, W:] = (part - high.astype(F32)).astype(BF)


def store_high(ref, real, imag):
    ref[:W, :W] = real.astype(BF)
    ref[W:, :W] = imag.astype(BF)


def product(left, right, dagger=False, high=False):
    if high:
        lhs = left[:, :W]
    else:
        whole = left[...]
        lhs = jnp.concatenate([whole, whole], 1)
    if dagger:
        up = right[:, :W]
        low = None if high else right[:, W:]
        rhs = up if high else jnp.concatenate([up, up, low, low], 1)
        dims = (((1,), (1,)), ((), ()))
    else:
        up = jnp.concatenate([right[:W, :W], right[W:, :W]], 1)
        if high:
            rhs = up
        else:
            low = jnp.concatenate([right[:W, W:], right[W:, W:]], 1)
            rhs = jnp.concatenate([up, up, low, low], 0)
        dims = (((1,), (0,)), ((), ()))
    full = lax.dot_general(lhs, rhs, dims, preferred_element_type=F32)
    if dagger:
        return full[:W, :W] + full[W:, W:], full[W:, :W] - full[:W, W:]
    return full[:W, :W] - full[W:, W:], full[:W, W:] + full[W:, :W]


def kernel(
    where_ref, scal_ref, sig_ref, ham_ref, hop_ref,
    less_ref, great_ref, flow_ref,
    hop_f, sys_f, inv_f, tmp_f, inj_f, gr_f, t_f, l_f, full_f,
    inv, gl, gr, folded_r, folded_l,
):
    count = sig_ref.shape[2]
    slabs = ham_ref.shape[0]
    energies = range(count)
    rows = lax.broadcasted_iota(jnp.int32, (W, W), 0)
    cols = lax.broadcasted_iota(jnp.int32, (W, W), 1)
    eye = jnp.where(rows == cols, 1.0, 0.0).astype(F32)
    here = where_ref[0]

    def unpack(value):
        turned = value.T
        real = jnp.where(rows < cols, value, jnp.where(rows > cols, -turned, 0.0))
        imag = jnp.where(rows >= cols, value, turned)
        return real, imag

    store(hop_f, hop_ref[0].T, -hop_ref[1].T)

    def forward(slab, last):
        place = lax.rem(slab - here + slabs, slabs)
        at_left = jnp.where(slab == 0, 1.0, 0.0)
        norms = []
        for e in energies:
            less = unpack(sig_ref[place, 0, e])
            great = unpack(sig_ref[place, 1, e])
            fill = scal_ref[2, e] if last else at_left * scal_ref[1, e]
            contact = contact_rate if last else at_left * contact_rate
            sys_r = scal_ref[0, e] * eye - ham_ref[slab, 0] - 0.5 * (great[0] - less[0])
            sys_i = (broaden + contact) * eye - ham_ref[slab, 1] - 0.5 * (great[1] - less[1])
            inj_r = less[0]
            inj_i = less[1] + 2.0 * contact_rate * fill * eye
            if not last:
                sys_r = sys_r - folded_r[e, 0]
                sys_i = sys_i - folded_r[e, 1]
                inj_r = inj_r + folded_l[e, 0]
                inj_i = inj_i + folded_l[e, 1]
            store(sys_f.at[e], sys_r, sys_i)
            store(inj_f.at[e], inj_r, inj_i)
            back_r = sys_r.T
            back_i = -sys_i.T
            inv[e, 0] = back_r
            inv[e, 1] = back_i
            store_high(inv_f.at[e], back_r, back_i)
        for e in energies:
            real, imag = product(inv_f.at[e], sys_f.at[e], high=True)
            norms.append(jnp.sum(jnp.sqrt(real * real + imag * imag), axis=0, keepdims=True))
        bound = functools.reduce(jnp.maximum, norms)
        bound = 1.05 * jnp.max(bound)
        scale = 1.0 / bound
        for e in energies:
            real = inv[e, 0] * scale
            imag = inv[e, 1] * scale
            inv[e, 0] = real
            inv[e, 1] = imag
            store_high(inv_f.at[e], real, imag)

        def grow(carry):
            lowest, done = carry
            used = jnp.maximum(lowest, LEAST)
            a = 4.0 / (1.0 + used)
            b = a / (1.0 + used)
            after = jnp.minimum(lowest * (a - b * lowest), b * used)
            centre = jnp.where(after >= 0.9, 2.0 / (1.0 + after), 1.0)
            for e in energies:
                real, imag = product(inv_f.at[e], sys_f.at[e], high=True)
                store_high(tmp_f.at[e], real, imag)
            for e in energies:
                real, imag = product(tmp_f.at[e], inv_f.at[e], high=True)
                real = centre * (a * inv[e, 0] - b * real)
                imag = centre * (a * inv[e, 1] - b * imag)
                inv[e, 0] = real
                inv[e, 1] = imag
                store_high(inv_f.at[e], real, imag)
            return after, done + 1

        lax.while_loop(
            lambda carry: jnp.logical_and(carry[0] < 0.9, carry[1] < 64),
            grow,
            (broaden * broaden * scale, jnp.int32(0)),
        )
        for e in energies:
            store(inv_f.at[e], inv[e, 0], inv[e, 1])

        def refine(carry):
            sizes = []
            for e in energies:
                real, imag = product(inv_f.at[e], sys_f.at[e])
                real = eye - real
                sizes.append(jnp.sum(real * real + imag * imag, axis=0, keepdims=True))
                store_high(tmp_f.at[e], real, -imag)
            for e in energies:
                real, imag = product(tmp_f.at[e], inv_f.at[e], high=True)
                real = inv[e, 0] + real
                imag = inv[e, 1] + imag
                inv[e, 0] = real
                inv[e, 1] = imag
                store(inv_f.at[e], real, imag)
            return jnp.max(functools.reduce(jnp.maximum, [jnp.sum(size) for size in sizes])), carry[1] + 1

        lax.while_loop(
            lambda carry: jnp.logical_and(carry[0] > 4.0e-6, carry[1] < 24),
            refine,
            (jnp.float32(1.0), jnp.int32(0)),
        )
        for e in energies:
            gr[slab, e, 0] = inv[e, 0]
            gr[slab, e, 1] = inv[e, 1]
            store(gr_f.at[slab, e], inv[e, 0], inv[e, 1])
            real, imag = product(inv_f.at[e], inj_f.at[e])
            store(tmp_f.at[e], real, imag)
        for e in energies:
            real, imag = product(tmp_f.at[e], inv_f.at[e], dagger=True)
            gl[slab, e, 0] = real
            gl[slab, e, 1] = imag
            store(inj_f.at[e], real, imag)

    def fold(slab):
        for e in energies:
            real, imag = product(hop_f, gr_f.at[slab, e])
            store(t_f.at[slab, e], real, imag)
            real, imag = product(hop_f, inj_f.at[e])
            store(l_f.at[slab, e], real, imag)
        for e in energies:
            real, imag = product(t_f.at[slab, e], hop_f, dagger=True)
            folded_r[e, 0] = real
            folded_r[e, 1] = imag
            real, imag = product(l_f.at[slab, e], hop_f, dagger=True)
            folded_l[e, 0] = real
            folded_l[e, 1] = imag

    forward(slabs - 1, True)

    def down(step, carry):
        slab = slabs - 2 - step
        fold(slab + 1)
        forward(slab, False)
        return carry

    lax.fori_loop(0, slabs - 1, down, 0)

    def finish(slab, e, green, less):
        less_ref[e, slab, 0] = less[0]
        less_ref[e, slab, 1] = less[1]
        great_r = less[0] + green[0] - green[0].T
        great_i = less[1] + green[1] + green[1].T
        great_ref[e, slab, 0] = great_r
        great_ref[e, slab, 1] = great_i
        return great_i

    flow = jnp.zeros((1, W), F32)
    for e in energies:
        green = (gr[0, e, 0], gr[0, e, 1])
        less = (gl[0, e, 0], gl[0, e, 1])
        great_i = finish(0, e, green, less)
        fill = scal_ref[1, e]
        mixed = fill * great_i + (1.0 - fill) * less[1]
        flow = flow - jnp.sum(jnp.where(rows == cols, mixed, 0.0), axis=0, keepdims=True)
        store(full_f.at[0, e], *green)
        store(full_f.at[1, e], *less)
    flow_ref[...] = jnp.broadcast_to(jnp.sum(flow, axis=1, keepdims=True), flow_ref.shape)

    def up(slab, carry):
        for e in energies:
            real, imag = product(gr_f.at[slab, e], hop_f, dagger=True)
            store(sys_f.at[e], real, imag)
        for e in energies:
            real, imag = product(sys_f.at[e], full_f.at[0, e])
            store(tmp_f.at[e], real, imag)
            real, imag = product(sys_f.at[e], full_f.at[1, e])
            store(inj_f.at[e], real, imag)
        for e in energies:
            real, imag = product(tmp_f.at[e], t_f.at[slab, e])
            green = (gr[slab, e, 0] + real, gr[slab, e, 1] + imag)
            cross = product(tmp_f.at[e], l_f.at[slab, e])
            real, imag = product(inj_f.at[e], sys_f.at[e], dagger=True)
            less = (
                gl[slab, e, 0] + real + cross[0] - cross[0].T,
                gl[slab, e, 1] + imag + cross[1] + cross[1].T,
            )
            finish(slab, e, green, less)
            store(full_f.at[0, e], *green)
            store(full_f.at[1, e], *less)
        return carry

    lax.fori_loop(1, slabs, up, 0)


def transport(place, scalars, sigma, hamiltonian, coupling):
    slabs, _, count = sigma.shape[:3]
    form = (2 * W, 2 * W)
    vmem = pl.BlockSpec(memory_space=pltpu.VMEM)
    smem = pl.BlockSpec(memory_space=pltpu.SMEM)
    blocks = jax.ShapeDtypeStruct((count, slabs, 2, W, W), F32)
    return pl.pallas_call(
        kernel,
        out_shape=(blocks, blocks, jax.ShapeDtypeStruct((8, W), F32)),
        in_specs=[smem, smem, vmem, vmem, vmem],
        out_specs=(vmem, vmem, vmem),
        scratch_shapes=[
            pltpu.VMEM(form, BF),
            pltpu.VMEM((count,) + form, BF),
            pltpu.VMEM((count,) + form, BF),
            pltpu.VMEM((count,) + form, BF),
            pltpu.VMEM((count,) + form, BF),
            pltpu.VMEM((slabs, count) + form, BF),
            pltpu.VMEM((slabs, count) + form, BF),
            pltpu.VMEM((slabs, count) + form, BF),
            pltpu.VMEM((2, count) + form, BF),
            pltpu.VMEM((count, 2, W, W), F32),
            pltpu.VMEM((slabs, count, 2, W, W), F32),
            pltpu.VMEM((slabs, count, 2, W, W), F32),
            pltpu.VMEM((count, 2, W, W), F32),
            pltpu.VMEM((count, 2, W, W), F32),
        ],
        compiler_params=pltpu.CompilerParams(vmem_limit_bytes=48 * 1024 * 1024),
        cost_estimate=pl.CostEstimate(flops=20_000_000_000, bytes_accessed=8_000_000, transcendentals=0),
    )(place, scalars, sigma, hamiltonian, coupling)


def moved(array, axis, by):
    size = lax.axis_size(axis)
    return lax.ppermute(array, axis, [(i, (i + by) % size) for i in range(size)])


def block(array, index):
    return lax.dynamic_index_in_dim(array, index, 0, keepdims=False)


def onward(field, upward):
    blank = jnp.zeros_like(field[:1])
    if upward:
        return jnp.concatenate([field[1:], blank], 0)
    return jnp.concatenate([blank, field[:-1]], 0)


def shards(lesser, greater, hamiltonian, coupling, shift, phonon_weight):
    n_energy = lax.axis_size("energy")
    n_mom = lax.axis_size("mom")
    here = lax.axis_index("energy")
    me = lax.axis_index("mom")
    count = lesser.shape[0]
    total = count * n_energy
    upper = jnp.triu(jnp.ones((W, W), jnp.bool_), 1)

    def packed(field):
        field = field[:, 0, 0]
        return jnp.swapaxes(jnp.where(upper, field[:, :, 0], field[:, :, 1]), 0, 1)

    less = packed(lesser)
    great = packed(greater)
    after, before, across = (me + 1) % n_mom, (me + n_mom - 1) % n_mom, (me + 2) % n_mom
    first_a = moved(block(less, across), "mom", 1)
    first_b = moved(block(great, across), "mom", -1)
    second_a = moved(jnp.stack([block(less, after) + first_a, block(great, after)]), "mom", 1)
    second_b = moved(jnp.stack([block(less, before), block(great, before) + first_b]), "mom", -1)
    summed = jnp.stack([block(less, me), block(great, me)]) + (second_a + second_b)

    def exchange(by):
        def branch(field):
            return moved(field, "energy", -by), moved(field, "energy", by)

        return branch

    amount = shift[0]
    higher, beneath = lax.switch(amount - 1, [exchange(k + 1) for k in range(SMAX)], summed)
    along = jax.vmap(functools.partial(onward, upward=True))
    back = jax.vmap(functools.partial(onward, upward=False))
    higher = jnp.where(here + amount >= n_energy, along(higher), higher) * (1.0 / n_mom)
    beneath = jnp.where(here - amount < 0, back(beneath), beneath) * (1.0 / n_mom)
    emission = phonon_weight[0]
    absorption = phonon_weight[1]
    share = jnp.stack(
        [
            emission * higher[0] + absorption * beneath[0],
            emission * beneath[1] + absorption * higher[1],
        ]
    )
    from_before = moved(share, "mom", 1)
    from_after = moved(share, "mom", -1)
    far_less = moved(from_before[0], "mom", 1)
    far_great = moved(from_after[1], "mom", -1)
    sigma = jnp.stack([share, from_after, jnp.stack([far_less, far_great]), from_before])

    grid = (jnp.arange(count) * n_energy + here).astype(F32)
    energy = (grid + 0.5) * (2.0 * band_edge / total) - band_edge
    scalars = jnp.stack(
        [
            energy,
            jax.nn.sigmoid((left_level - energy) / thermal),
            jax.nn.sigmoid((right_level - energy) / thermal),
        ]
    )
    place = jnp.reshape(me, (1,)).astype(jnp.int32)
    less_new, great_new, flow = transport(place, scalars, sigma, hamiltonian[0], coupling[0])
    current = lax.psum(flow[0, 0] * (2.0 * band_edge / total), ("energy", "mom"))
    return (less_new[:, None, None], great_new[:, None, None], current)


def solution(mesh):
    return jax.shard_map(
        shards,
        mesh=mesh,
        in_specs=(
            P(None, "energy", "mom", None, None, None, None),
            P(None, "energy", "mom", None, None, None, None),
            P("mom", None, None, None, None),
            P("mom", None, None, None),
            P(),
            P(),
        ),
        out_specs=(
            P(None, "energy", "mom", None, None, None, None),
            P(None, "energy", "mom", None, None, None, None),
            P(),
        ),
        check_vma=False,
    )
```

```python
import functools

import jax
import jax.numpy as jnp
from jax import lax
from jax.experimental import pallas as pl
from jax.experimental.pallas import tpu as pltpu
from jax.sharding import PartitionSpec as P

SMAX = 7
broaden = 0.2
contact_rate = 0.5
left_level = 0.3
right_level = -0.3
thermal = 0.1
band_edge = 2.0

W = 128
BF = jnp.bfloat16
F32 = jnp.float32
LEAST = 0.03


def store(ref, real, imag):
    for row, part in ((0, real), (W, imag)):
        high = part.astype(BF)
        ref[row : row + W, :W] = high
        ref[row : row + W, W:] = (part - high.astype(F32)).astype(BF)


def store_high(ref, real, imag):
    ref[:W, :W] = real.astype(BF)
    ref[W:, :W] = imag.astype(BF)


def product(left, right, dagger=False, high=False):
    if high:
        lhs = left[:, :W]
    else:
        whole = left[...]
        lhs = jnp.concatenate([whole, whole], 1)
    if dagger:
        up = right[:, :W]
        low = None if high else right[:, W:]
        rhs = up if high else jnp.concatenate([up, up, low, low], 1)
        dims = (((1,), (1,)), ((), ()))
    else:
        up = jnp.concatenate([right[:W, :W], right[W:, :W]], 1)
        if high:
            rhs = up
        else:
            low = jnp.concatenate([right[:W, W:], right[W:, W:]], 1)
            rhs = jnp.concatenate([up, up, low, low], 0)
        dims = (((1,), (0,)), ((), ()))
    full = lax.dot_general(lhs, rhs, dims, preferred_element_type=F32)
    if dagger:
        return full[:W, :W] + full[W:, W:], full[W:, :W] - full[:W, W:]
    return full[:W, :W] - full[W:, W:], full[:W, W:] + full[W:, :W]


def kernel(
    scal_ref, sig_ref, ham_ref, hop_ref,
    less_ref, great_ref, flow_ref,
    hop_f, sys_f, inv_f, tmp_f, inj_f, gr_f, t_f, l_f, full_f,
    inv, gl, gr, folded_r, folded_l,
):
    count = sig_ref.shape[2]
    slabs = ham_ref.shape[0]
    energies = range(count)
    rows = lax.broadcasted_iota(jnp.int32, (W, W), 0)
    cols = lax.broadcasted_iota(jnp.int32, (W, W), 1)
    eye = jnp.where(rows == cols, 1.0, 0.0).astype(F32)

    def unpack(value):
        turned = value.T
        real = jnp.where(rows < cols, value, jnp.where(rows > cols, -turned, 0.0))
        imag = jnp.where(rows >= cols, value, turned)
        return real, imag

    store(hop_f, hop_ref[0].T, -hop_ref[1].T)

    def forward(slab, last):
        at_left = jnp.where(slab == 0, 1.0, 0.0)
        norms = []
        for e in energies:
            less = unpack(sig_ref[slab, 0, e])
            great = unpack(sig_ref[slab, 1, e])
            fill = scal_ref[2, e] if last else at_left * scal_ref[1, e]
            contact = contact_rate if last else at_left * contact_rate
            sys_r = scal_ref[0, e] * eye - ham_ref[slab, 0] - 0.5 * (great[0] - less[0])
            sys_i = (broaden + contact) * eye - ham_ref[slab, 1] - 0.5 * (great[1] - less[1])
            inj_r = less[0]
            inj_i = less[1] + 2.0 * contact_rate * fill * eye
            if not last:
                sys_r = sys_r - folded_r[e, 0]
                sys_i = sys_i - folded_r[e, 1]
                inj_r = inj_r + folded_l[e, 0]
                inj_i = inj_i + folded_l[e, 1]
            store(sys_f.at[e], sys_r, sys_i)
            store(inj_f.at[e], inj_r, inj_i)
            back_r = sys_r.T
            back_i = -sys_i.T
            inv[e, 0] = back_r
            inv[e, 1] = back_i
            store_high(inv_f.at[e], back_r, back_i)
        for e in energies:
            real, imag = product(inv_f.at[e], sys_f.at[e], high=True)
            norms.append(jnp.sum(jnp.sqrt(real * real + imag * imag), axis=0, keepdims=True))
        bound = functools.reduce(jnp.maximum, norms)
        bound = 1.05 * jnp.max(bound)
        scale = 1.0 / bound
        for e in energies:
            real = inv[e, 0] * scale
            imag = inv[e, 1] * scale
            inv[e, 0] = real
            inv[e, 1] = imag
            store_high(inv_f.at[e], real, imag)

        def grow(carry):
            lowest, done = carry
            used = jnp.maximum(lowest, LEAST)
            a = 4.0 / (1.0 + used)
            b = a / (1.0 + used)
            after = jnp.minimum(lowest * (a - b * lowest), b * used)
            centre = jnp.where(after >= 0.9, 2.0 / (1.0 + after), 1.0)
            for e in energies:
                real, imag = product(inv_f.at[e], sys_f.at[e], high=True)
                store_high(tmp_f.at[e], real, imag)
            for e in energies:
                real, imag = product(tmp_f.at[e], inv_f.at[e], high=True)
                real = centre * (a * inv[e, 0] - b * real)
                imag = centre * (a * inv[e, 1] - b * imag)
                inv[e, 0] = real
                inv[e, 1] = imag
                store_high(inv_f.at[e], real, imag)
            return after, done + 1

        lax.while_loop(
            lambda carry: jnp.logical_and(carry[0] < 0.9, carry[1] < 64),
            grow,
            (broaden * broaden * scale, jnp.int32(0)),
        )
        for e in energies:
            store(inv_f.at[e], inv[e, 0], inv[e, 1])

        def refine(carry):
            sizes = []
            for e in energies:
                real, imag = product(inv_f.at[e], sys_f.at[e])
                real = eye - real
                sizes.append(jnp.sum(real * real + imag * imag, axis=0, keepdims=True))
                store_high(tmp_f.at[e], real, -imag)
            for e in energies:
                real, imag = product(tmp_f.at[e], inv_f.at[e], high=True)
                real = inv[e, 0] + real
                imag = inv[e, 1] + imag
                inv[e, 0] = real
                inv[e, 1] = imag
                store(inv_f.at[e], real, imag)
            return jnp.max(functools.reduce(jnp.maximum, [jnp.sum(size) for size in sizes])), carry[1] + 1

        lax.while_loop(
            lambda carry: jnp.logical_and(carry[0] > 4.0e-6, carry[1] < 24),
            refine,
            (jnp.float32(1.0), jnp.int32(0)),
        )
        for e in energies:
            gr[slab, e, 0] = inv[e, 0]
            gr[slab, e, 1] = inv[e, 1]
            store(gr_f.at[slab, e], inv[e, 0], inv[e, 1])
            real, imag = product(inv_f.at[e], inj_f.at[e])
            store(tmp_f.at[e], real, imag)
        for e in energies:
            real, imag = product(tmp_f.at[e], inv_f.at[e], dagger=True)
            gl[slab, e, 0] = real
            gl[slab, e, 1] = imag
            store(inj_f.at[e], real, imag)

    def fold(slab):
        for e in energies:
            real, imag = product(hop_f, gr_f.at[slab, e])
            store(t_f.at[slab, e], real, imag)
            real, imag = product(hop_f, inj_f.at[e])
            store(l_f.at[slab, e], real, imag)
        for e in energies:
            real, imag = product(t_f.at[slab, e], hop_f, dagger=True)
            folded_r[e, 0] = real
            folded_r[e, 1] = imag
            real, imag = product(l_f.at[slab, e], hop_f, dagger=True)
            folded_l[e, 0] = real
            folded_l[e, 1] = imag

    forward(slabs - 1, True)

    def down(step, carry):
        slab = slabs - 2 - step
        fold(slab + 1)
        forward(slab, False)
        return carry

    lax.fori_loop(0, slabs - 1, down, 0)

    def finish(slab, e, green, less):
        less_ref[e, slab, 0] = less[0]
        less_ref[e, slab, 1] = less[1]
        great_r = less[0] + green[0] - green[0].T
        great_i = less[1] + green[1] + green[1].T
        great_ref[e, slab, 0] = great_r
        great_ref[e, slab, 1] = great_i
        return great_i

    flow = jnp.zeros((1, W), F32)
    for e in energies:
        green = (gr[0, e, 0], gr[0, e, 1])
        less = (gl[0, e, 0], gl[0, e, 1])
        great_i = finish(0, e, green, less)
        fill = scal_ref[1, e]
        mixed = fill * great_i + (1.0 - fill) * less[1]
        flow = flow - jnp.sum(jnp.where(rows == cols, mixed, 0.0), axis=0, keepdims=True)
        store(full_f.at[0, e], *green)
        store(full_f.at[1, e], *less)
    flow_ref[...] = jnp.broadcast_to(jnp.sum(flow, axis=1, keepdims=True), flow_ref.shape)

    def up(slab, carry):
        for e in energies:
            real, imag = product(gr_f.at[slab, e], hop_f, dagger=True)
            store(sys_f.at[e], real, imag)
        for e in energies:
            real, imag = product(sys_f.at[e], full_f.at[0, e])
            store(tmp_f.at[e], real, imag)
            real, imag = product(sys_f.at[e], full_f.at[1, e])
            store(inj_f.at[e], real, imag)
        for e in energies:
            real, imag = product(tmp_f.at[e], t_f.at[slab, e])
            green = (gr[slab, e, 0] + real, gr[slab, e, 1] + imag)
            cross = product(tmp_f.at[e], l_f.at[slab, e])
            real, imag = product(inj_f.at[e], sys_f.at[e], dagger=True)
            less = (
                gl[slab, e, 0] + real + cross[0] - cross[0].T,
                gl[slab, e, 1] + imag + cross[1] + cross[1].T,
            )
            finish(slab, e, green, less)
            store(full_f.at[0, e], *green)
            store(full_f.at[1, e], *less)
        return carry

    lax.fori_loop(1, slabs, up, 0)


def transport(scalars, sigma, hamiltonian, coupling):
    slabs, _, count = sigma.shape[:3]
    form = (2 * W, 2 * W)
    vmem = pl.BlockSpec(memory_space=pltpu.VMEM)
    smem = pl.BlockSpec(memory_space=pltpu.SMEM)
    blocks = jax.ShapeDtypeStruct((count, slabs, 2, W, W), F32)
    return pl.pallas_call(
        kernel,
        out_shape=(blocks, blocks, jax.ShapeDtypeStruct((8, W), F32)),
        in_specs=[smem, vmem, vmem, vmem],
        out_specs=(vmem, vmem, vmem),
        scratch_shapes=[
            pltpu.VMEM(form, BF),
            pltpu.VMEM((count,) + form, BF),
            pltpu.VMEM((count,) + form, BF),
            pltpu.VMEM((count,) + form, BF),
            pltpu.VMEM((count,) + form, BF),
            pltpu.VMEM((slabs, count) + form, BF),
            pltpu.VMEM((slabs, count) + form, BF),
            pltpu.VMEM((slabs, count) + form, BF),
            pltpu.VMEM((2, count) + form, BF),
            pltpu.VMEM((count, 2, W, W), F32),
            pltpu.VMEM((slabs, count, 2, W, W), F32),
            pltpu.VMEM((slabs, count, 2, W, W), F32),
            pltpu.VMEM((count, 2, W, W), F32),
            pltpu.VMEM((count, 2, W, W), F32),
        ],
        compiler_params=pltpu.CompilerParams(vmem_limit_bytes=48 * 1024 * 1024),
        cost_estimate=pl.CostEstimate(flops=20_000_000_000, bytes_accessed=8_000_000, transcendentals=0),
    )(scalars, sigma, hamiltonian, coupling)


MESH = pl.DeviceIdType.MESH
CHUNKS = 4


def exchange_kernel(
    by, n_energy, n_mom,
    weight_ref, less_ref, great_ref, sigma_ref,
    pack, near_a, near_b, half_a, half_b, share, high, low, send_sem, recv_sem,
):
    place = lax.axis_index("energy")
    me = lax.axis_index("mom")
    count = less_ref.shape[0]
    depth = W // CHUNKS
    after = lax.rem(me + 1, n_mom)
    before = lax.rem(me + n_mom - 1, n_mom)
    across = lax.rem(me + 2, n_mom)
    over = {"energy": lax.rem(place + by, n_energy)}
    under = {"energy": lax.rem(place - by + n_energy, n_energy)}
    wrapped_up = lax.div(place + by, n_energy)
    wrapped_down = 1 - lax.div(place - by + n_energy, n_energy)
    kept_up = (1 - wrapped_up).astype(F32)
    kept_down = (1 - wrapped_down).astype(F32)
    emission = weight_ref[0] * (1.0 / n_mom)
    absorption = weight_ref[1] * (1.0 / n_mom)

    barrier = pltpu.get_barrier_semaphore()
    for peer in ({"mom": after}, {"mom": before}, over, under):
        pl.semaphore_signal(barrier, inc=1, device_id=peer, device_id_type=MESH)

    def send(kind, chunk, source, target, peer):
        copy = pltpu.make_async_remote_copy(
            src_ref=source,
            dst_ref=target,
            send_sem=send_sem.at[kind, chunk],
            recv_sem=recv_sem.at[kind, chunk],
            device_id=peer,
            device_id_type=MESH,
        )
        copy.start()
        return copy

    sent = {}
    rows = lax.broadcasted_iota(jnp.int32, (depth, W), 0)
    cols = lax.broadcasted_iota(jnp.int32, (depth, W), 1)
    for c in range(CHUNKS):
        span = slice(c * depth, (c + 1) * depth)
        upper = cols > rows + c * depth
        for slab in range(n_mom):
            for kind, ref in enumerate((less_ref, great_ref)):
                pack[c, slab, kind] = jnp.where(upper, ref[:, slab, 0, span], ref[:, slab, 1, span])
        if c == 0:
            pl.semaphore_wait(barrier, 4)
        sent[0, c] = send(0, c, pack.at[c, across, 0], near_a.at[c], {"mom": after})
        sent[1, c] = send(1, c, pack.at[c, across, 1], near_b.at[c], {"mom": before})
    for c in range(CHUNKS):
        sent[0, c].wait_recv()
        pack[c, after, 0] = pack[c, after, 0] + near_a[c]
        sent[1, c].wait_recv()
        pack[c, before, 1] = pack[c, before, 1] + near_b[c]
        sent[2, c] = send(2, c, pack.at[c, after], half_a.at[c], {"mom": after})
        sent[3, c] = send(3, c, pack.at[c, before], half_b.at[c], {"mom": before})
    for c in range(CHUNKS):
        sent[2, c].wait_recv()
        sent[3, c].wait_recv()
        share[c] = pack[c, me] + (half_a[c] + half_b[c])
        sent[4, c] = send(4, c, share.at[c], high.at[c], under)
        sent[5, c] = send(5, c, share.at[c], low.at[c], over)
    for c in range(CHUNKS):
        span = slice(c * depth, (c + 1) * depth)
        sent[4, c].wait_recv()
        sent[5, c].wait_recv()
        for j in range(count):
            if j < count - 1:
                up = [high[c, kind, j + wrapped_up] for kind in range(2)]
            else:
                up = [high[c, kind, j] * kept_up for kind in range(2)]
            if j > 0:
                down = [low[c, kind, j - wrapped_down] for kind in range(2)]
            else:
                down = [low[c, kind, j] * kept_down for kind in range(2)]
            sigma_ref[me, 0, j, span] = emission * up[0] + absorption * down[0]
            sigma_ref[me, 1, j, span] = emission * down[1] + absorption * up[1]
        mine = sigma_ref.at[me, :, :, span]
        sent[6, c] = send(6, c, mine, mine, {"mom": after})
        sent[7, c] = send(7, c, mine, mine, {"mom": before})
    for c in range(CHUNKS):
        span = slice(c * depth, (c + 1) * depth)
        sent[6, c].wait_recv()
        part = sigma_ref.at[before, 0, :, span]
        sent[8, c] = send(8, c, part, part, {"mom": after})
        sent[7, c].wait_recv()
        part = sigma_ref.at[after, 1, :, span]
        sent[9, c] = send(9, c, part, part, {"mom": before})
    for c in range(CHUNKS):
        sent[8, c].wait_recv()
        sent[9, c].wait_recv()
    for copy in sent.values():
        copy.wait_send()


def exchange(by, n_energy, n_mom, weight, lesser, greater):
    count = lesser.shape[0]
    depth = W // CHUNKS
    vmem = pl.BlockSpec(memory_space=pltpu.VMEM)
    half = (CHUNKS, count, depth, W)
    whole = (CHUNKS, 2, count, depth, W)
    return pl.pallas_call(
        functools.partial(exchange_kernel, by, n_energy, n_mom),
        out_shape=jax.ShapeDtypeStruct((n_mom, 2, count, W, W), F32),
        in_specs=[pl.BlockSpec(memory_space=pltpu.SMEM), vmem, vmem],
        out_specs=vmem,
        scratch_shapes=[
            pltpu.VMEM((CHUNKS, n_mom, 2, count, depth, W), F32),
            pltpu.VMEM(half, F32),
            pltpu.VMEM(half, F32),
            pltpu.VMEM(whole, F32),
            pltpu.VMEM(whole, F32),
            pltpu.VMEM(whole, F32),
            pltpu.VMEM(whole, F32),
            pltpu.VMEM(whole, F32),
            pltpu.SemaphoreType.DMA((10, CHUNKS)),
            pltpu.SemaphoreType.DMA((10, CHUNKS)),
        ],
        compiler_params=pltpu.CompilerParams(
            collective_id=by, has_side_effects=True, vmem_limit_bytes=32 * 1024 * 1024
        ),
    )(weight, lesser, greater)


def total_kernel(n_mom, flow_ref, total_ref, first, second, partial, send_sem, recv_sem):
    place = lax.axis_index("energy")
    me = lax.axis_index("mom")
    inner = second.shape[0]
    outer = first.shape[0]
    low = lax.rem(place, inner)
    high = lax.div(place, inner)
    slot = high * n_mom + me

    def outer_peer(step):
        other = lax.rem(slot + step, outer)
        return other, {"energy": lax.div(other, n_mom) * inner + low, "mom": lax.rem(other, n_mom)}

    def inner_peer(step):
        other = lax.rem(low + step, inner)
        return other, {"energy": high * inner + other, "mom": me}

    barrier = pltpu.get_barrier_semaphore()
    for step in range(1, outer):
        pl.semaphore_signal(barrier, inc=1, device_id=outer_peer(step)[1], device_id_type=MESH)
    for step in range(1, inner):
        pl.semaphore_signal(barrier, inc=1, device_id=inner_peer(step)[1], device_id_type=MESH)
    pl.semaphore_wait(barrier, outer + inner - 2)

    def round_of(source, slots, size, own, peer, base):
        def copy(index, step):
            return pltpu.make_async_remote_copy(
                src_ref=source,
                dst_ref=slots.at[index],
                send_sem=send_sem.at[base + step],
                recv_sem=recv_sem.at[base + index],
                device_id=peer(step)[1],
                device_id_type=MESH,
            )

        for step in range(1, size):
            copy(own, step).start()
        slots[own] = source[...]
        for step in range(1, size):
            copy(peer(step)[0], step).wait_recv()
        result = slots[0]
        for index in range(1, size):
            result = result + slots[index]
        for step in range(1, size):
            copy(own, step).wait_send()
        return result

    partial[...] = round_of(flow_ref, first, outer, slot, outer_peer, 0)
    total_ref[...] = round_of(partial, second, inner, low, inner_peer, outer)


def summed(flow, n_energy, n_mom):
    inner = 8
    outer = n_energy // inner * n_mom
    vmem = pl.BlockSpec(memory_space=pltpu.VMEM)
    return pl.pallas_call(
        functools.partial(total_kernel, n_mom),
        out_shape=jax.ShapeDtypeStruct(flow.shape, F32),
        in_specs=[vmem],
        out_specs=vmem,
        scratch_shapes=[
            pltpu.VMEM((outer,) + flow.shape, F32),
            pltpu.VMEM((inner,) + flow.shape, F32),
            pltpu.VMEM(flow.shape, F32),
            pltpu.SemaphoreType.DMA((outer + inner,)),
            pltpu.SemaphoreType.DMA((outer + inner,)),
        ],
        compiler_params=pltpu.CompilerParams(collective_id=SMAX + 1, has_side_effects=True),
    )(flow)


def shards(lesser, greater, hamiltonian, coupling, shift, phonon_weight):
    n_energy = lax.axis_size("energy")
    n_mom = lax.axis_size("mom")
    here = lax.axis_index("energy")
    count = lesser.shape[0]
    total = count * n_energy
    branches = [functools.partial(exchange, k + 1, n_energy, n_mom) for k in range(SMAX)]
    sigma = lax.switch(shift[0] - 1, branches, phonon_weight, lesser[:, 0, 0], greater[:, 0, 0])
    grid = (jnp.arange(count) * n_energy + here).astype(F32)
    energy = (grid + 0.5) * (2.0 * band_edge / total) - band_edge
    scalars = jnp.stack(
        [
            energy,
            jax.nn.sigmoid((left_level - energy) / thermal),
            jax.nn.sigmoid((right_level - energy) / thermal),
        ]
    )
    less_new, great_new, flow = transport(scalars, sigma, hamiltonian[0], coupling[0])
    current = summed(flow, n_energy, n_mom)[0, 0] * (2.0 * band_edge / total)
    return (less_new[:, None, None], great_new[:, None, None], current)


def solution(mesh):
    return jax.shard_map(
        shards,
        mesh=mesh,
        in_specs=(
            P(None, "energy", "mom", None, None, None, None),
            P(None, "energy", "mom", None, None, None, None),
            P("mom", None, None, None, None),
            P("mom", None, None, None),
            P(),
            P(),
        ),
        out_specs=(
            P(None, "energy", "mom", None, None, None, None),
            P(None, "energy", "mom", None, None, None, None),
            P(),
        ),
        check_vma=False,
    )
```

```python
import functools

import jax
import jax.numpy as jnp
from jax import lax
from jax.experimental import pallas as pl
from jax.experimental.pallas import tpu as pltpu
from jax.sharding import PartitionSpec as P

SMAX = 7
broaden = 0.2
contact_rate = 0.5
left_level = 0.3
right_level = -0.3
thermal = 0.1
band_edge = 2.0

W = 128
BF = jnp.bfloat16
F32 = jnp.float32
LEAST = 0.03


def store(ref, real, imag):
    for row, part in ((0, real), (W, imag)):
        high = part.astype(BF)
        ref[row : row + W, :W] = high
        ref[row : row + W, W:] = (part - high.astype(F32)).astype(BF)


def store_high(ref, real, imag):
    ref[:W, :W] = real.astype(BF)
    ref[W:, :W] = imag.astype(BF)


def product(left, right, dagger=False, high=False):
    if high:
        lhs = left[:, :W]
    else:
        whole = left[...]
        lhs = jnp.concatenate([whole, whole], 1)
    if dagger:
        up = right[:, :W]
        low = None if high else right[:, W:]
        rhs = up if high else jnp.concatenate([up, up, low, low], 1)
        dims = (((1,), (1,)), ((), ()))
    else:
        up = jnp.concatenate([right[:W, :W], right[W:, :W]], 1)
        if high:
            rhs = up
        else:
            low = jnp.concatenate([right[:W, W:], right[W:, W:]], 1)
            rhs = jnp.concatenate([up, up, low, low], 0)
        dims = (((1,), (0,)), ((), ()))
    full = lax.dot_general(lhs, rhs, dims, preferred_element_type=F32)
    if dagger:
        return full[:W, :W] + full[W:, W:], full[W:, :W] - full[:W, W:]
    return full[:W, :W] - full[W:, W:], full[:W, W:] + full[W:, :W]


FAST_LOW = 0.006
FAST_TOP = 0.4
FAST_GROW = 5
FAST_REFINE = 2
RESIDUAL = 1.0e-4


def schedule():
    lowest, steps = FAST_LOW, []
    for step in range(FAST_GROW):
        used = max(lowest, LEAST)
        a = 4.0 / (1.0 + used)
        b = a / (1.0 + used)
        lowest = min(lowest * (a - b * lowest), b * used)
        centre = 2.0 / (1.0 + lowest) if step == FAST_GROW - 1 else 1.0
        steps.append((a * centre, b * centre))
    return steps


class Solver:
    names = (
        "hop_f", "sys_f", "inv_f", "tmp_f", "inj_f", "gr_f", "t_f", "l_f", "full_f",
        "inv", "gl", "gr", "folded_r", "folded_l", "rho",
    )

    def __init__(self, fast, sigma, scal, ham, less, great, scratch, base=0):
        self.fast = fast
        self.sigma = sigma
        self.scal = lambda row, e: scal[row, base + e]
        self.ham = ham
        self.less = less
        self.great = great
        for name, ref in zip(self.names, scratch, strict=True):
            setattr(self, name, ref)
        self.count = self.inv.shape[0]
        self.slabs = ham.shape[0]
        self.energies = range(self.count)
        self.rows = lax.broadcasted_iota(jnp.int32, (W, W), 0)
        self.cols = lax.broadcasted_iota(jnp.int32, (W, W), 1)
        self.eye = jnp.where(self.rows == self.cols, 1.0, 0.0).astype(F32)

    @classmethod
    def scratch(cls, count, slabs):
        form = (2 * W, 2 * W)
        blocks = (count, 2, W, W)
        few = pltpu.VMEM((count,) + form, BF)
        many = pltpu.VMEM((slabs, count) + form, BF)
        every = pltpu.VMEM((slabs,) + blocks, F32)
        own = pltpu.VMEM(blocks, F32)
        return [
            pltpu.VMEM(form, BF), few, few, few, few, many, many, many,
            pltpu.VMEM((2, count) + form, BF), own, every, every, own, own, pltpu.VMEM((8, W), F32),
        ]

    def start(self, hop):
        store(self.hop_f, hop[0].T, -hop[1].T)
        self.rho[...] = jnp.zeros((8, W), F32)

    def block(self, slab, kind, e):
        value = self.sigma(slab, kind, e)
        turned = value.T
        real = jnp.where(self.rows < self.cols, value, jnp.where(self.rows > self.cols, -turned, 0.0))
        imag = jnp.where(self.rows >= self.cols, value, turned)
        return real, imag

    def grow_step(self, a, b):
        for e in self.energies:
            real, imag = product(self.inv_f.at[e], self.sys_f.at[e], high=True)
            store_high(self.tmp_f.at[e], real, imag)
        for e in self.energies:
            real, imag = product(self.tmp_f.at[e], self.inv_f.at[e], high=True)
            real = a * self.inv[e, 0] - b * real
            imag = a * self.inv[e, 1] - b * imag
            self.inv[e, 0] = real
            self.inv[e, 1] = imag
            store_high(self.inv_f.at[e], real, imag)

    def whole_form(self):
        for e in self.energies:
            store(self.inv_f.at[e], self.inv[e, 0], self.inv[e, 1])

    def refine_step(self):
        sizes = []
        for e in self.energies:
            real, imag = product(self.inv_f.at[e], self.sys_f.at[e])
            real = self.eye - real
            sizes.append(jnp.sum(real * real + imag * imag, axis=0, keepdims=True))
            store_high(self.tmp_f.at[e], real, -imag)
        for e in self.energies:
            real, imag = product(self.tmp_f.at[e], self.inv_f.at[e], high=True)
            real = self.inv[e, 0] + real
            imag = self.inv[e, 1] + imag
            self.inv[e, 0] = real
            self.inv[e, 1] = imag
            store(self.inv_f.at[e], real, imag)
        return sizes

    def invert(self, midway):
        norms = []
        for e in self.energies:
            real, imag = product(self.inv_f.at[e], self.sys_f.at[e], high=True)
            norms.append(jnp.sum(jnp.sqrt(real * real + imag * imag), axis=0, keepdims=True))
            if self.fast:
                store_high(self.tmp_f.at[e], real, imag)
        bound = 1.05 * jnp.max(functools.reduce(jnp.maximum, norms))
        if self.fast:
            steps = schedule()
            scale = 1.0 / (FAST_TOP * bound)
            first = steps[0][0] * scale
            second = steps[0][1] * scale * scale
            for e in self.energies:
                real, imag = product(self.tmp_f.at[e], self.inv_f.at[e], high=True)
                real = first * self.inv[e, 0] - second * real
                imag = first * self.inv[e, 1] - second * imag
                self.inv[e, 0] = real
                self.inv[e, 1] = imag
                store_high(self.inv_f.at[e], real, imag)
            for place, (a, b) in enumerate(steps[1:]):
                self.grow_step(a, b)
                if place == 1 and midway is not None:
                    midway()
            self.whole_form()
            for step in range(FAST_REFINE):
                sizes = self.refine_step()
            self.rho[0:1] = self.rho[0:1] + functools.reduce(jnp.add, sizes)
            return
        scale = 1.0 / bound
        for e in self.energies:
            real = self.inv[e, 0] * scale
            imag = self.inv[e, 1] * scale
            self.inv[e, 0] = real
            self.inv[e, 1] = imag
        self.whole_form()

        def grow(carry):
            lowest, done = carry
            used = jnp.maximum(lowest, LEAST)
            a = 4.0 / (1.0 + used)
            b = a / (1.0 + used)
            after = jnp.minimum(lowest * (a - b * lowest), b * used)
            for e in self.energies:
                real, imag = product(self.inv_f.at[e], self.sys_f.at[e])
                store(self.tmp_f.at[e], real, imag)
            for e in self.energies:
                real, imag = product(self.tmp_f.at[e], self.inv_f.at[e])
                real = a * self.inv[e, 0] - b * real
                imag = a * self.inv[e, 1] - b * imag
                self.inv[e, 0] = real
                self.inv[e, 1] = imag
                store(self.inv_f.at[e], real, imag)
            return after, done + 1

        lax.while_loop(
            lambda carry: jnp.logical_and(carry[0] < 0.9, carry[1] < 64),
            grow,
            (broaden * broaden * scale, jnp.int32(0)),
        )

        def refine(carry):
            sizes = [jnp.sum(size) for size in self.refine_step()]
            return functools.reduce(jnp.maximum, sizes), carry[1] + 1

        lax.while_loop(
            lambda carry: jnp.logical_and(carry[0] > 4.0e-6, carry[1] < 24),
            refine,
            (jnp.float32(1.0), jnp.int32(0)),
        )

    def level(self, slab, last, midway=None):
        at_left = 0.0 if last else jnp.where(slab == 0, 1.0, 0.0)
        for e in self.energies:
            less = self.block(slab, 0, e)
            great = self.block(slab, 1, e)
            fill = self.scal(2, e) if last else at_left * self.scal(1, e)
            contact = contact_rate if last else at_left * contact_rate
            sys_r = self.scal(0, e) * self.eye - self.ham[slab, 0] - 0.5 * (great[0] - less[0])
            sys_i = (broaden + contact) * self.eye - self.ham[slab, 1] - 0.5 * (great[1] - less[1])
            inj_r = less[0]
            inj_i = less[1] + 2.0 * contact_rate * fill * self.eye
            if not last:
                sys_r = sys_r - self.folded_r[e, 0]
                sys_i = sys_i - self.folded_r[e, 1]
                inj_r = inj_r + self.folded_l[e, 0]
                inj_i = inj_i + self.folded_l[e, 1]
            store(self.sys_f.at[e], sys_r, sys_i)
            store(self.inj_f.at[e], inj_r, inj_i)
            back_r = sys_r.T
            back_i = -sys_i.T
            self.inv[e, 0] = back_r
            self.inv[e, 1] = back_i
            store_high(self.inv_f.at[e], back_r, back_i)
        self.invert(midway)
        for e in self.energies:
            self.gr[slab, e] = self.inv[e]
            self.gr_f[slab, e] = self.inv_f[e]
            real, imag = product(self.inv_f.at[e], self.inj_f.at[e])
            store(self.tmp_f.at[e], real, imag)
        for e in self.energies:
            real, imag = product(self.tmp_f.at[e], self.inv_f.at[e], dagger=True)
            self.gl[slab, e, 0] = real
            self.gl[slab, e, 1] = imag
            store(self.inj_f.at[e], real, imag)

    def fold(self, slab):
        for e in self.energies:
            real, imag = product(self.hop_f, self.gr_f.at[slab, e])
            store(self.t_f.at[slab, e], real, imag)
            real, imag = product(self.hop_f, self.inj_f.at[e])
            store(self.l_f.at[slab, e], real, imag)
        for e in self.energies:
            real, imag = product(self.t_f.at[slab, e], self.hop_f, dagger=True)
            self.folded_r[e, 0] = real
            self.folded_r[e, 1] = imag
            real, imag = product(self.l_f.at[slab, e], self.hop_f, dagger=True)
            self.folded_l[e, 0] = real
            self.folded_l[e, 1] = imag

    def flow(self):
        flow = jnp.zeros((1, W), F32)
        for e in self.energies:
            fill = self.scal(1, e)
            less = self.gl[0, e, 1]
            mixed = fill * (less + 2.0 * self.gr[0, e, 1]) + (1.0 - fill) * less
            flow = flow - jnp.sum(mixed * self.eye, axis=0, keepdims=True)
        flow = jnp.broadcast_to(jnp.sum(flow, axis=1, keepdims=True), (8, W))
        missed = jnp.broadcast_to(jnp.sum(self.rho[0:1], axis=1, keepdims=True), (8, W))
        missed = jnp.where(missed <= RESIDUAL, 0.0, 1.0)
        return jnp.where(lax.broadcasted_iota(jnp.int32, (8, W), 0) == 0, flow, missed)

    def finish(self, slab, e, green, less):
        self.less[e, slab, 0] = less[0]
        self.less[e, slab, 1] = less[1]
        self.great[e, slab, 0] = less[0] + green[0] - green[0].T
        self.great[e, slab, 1] = less[1] + green[1] + green[1].T
        store(self.full_f.at[0, e], *green)
        store(self.full_f.at[1, e], *less)

    def first(self):
        for e in self.energies:
            self.finish(0, e, (self.gr[0, e, 0], self.gr[0, e, 1]), (self.gl[0, e, 0], self.gl[0, e, 1]))

    def up(self, slab):
        for e in self.energies:
            real, imag = product(self.gr_f.at[slab, e], self.hop_f, dagger=True)
            store(self.sys_f.at[e], real, imag)
        for e in self.energies:
            real, imag = product(self.sys_f.at[e], self.full_f.at[0, e])
            store(self.tmp_f.at[e], real, imag)
            real, imag = product(self.sys_f.at[e], self.full_f.at[1, e])
            store(self.inj_f.at[e], real, imag)
        for e in self.energies:
            real, imag = product(self.tmp_f.at[e], self.t_f.at[slab, e])
            green = (self.gr[slab, e, 0] + real, self.gr[slab, e, 1] + imag)
            cross = product(self.tmp_f.at[e], self.l_f.at[slab, e])
            real, imag = product(self.inj_f.at[e], self.sys_f.at[e], dagger=True)
            less = (
                self.gl[slab, e, 0] + real + cross[0] - cross[0].T,
                self.gl[slab, e, 1] + imag + cross[1] + cross[1].T,
            )
            self.finish(slab, e, green, less)


def rows_of(sigma_ref):
    def read(slab, kind, e):
        return jnp.concatenate([sigma_ref[slab, owner, kind, e] for owner in range(sigma_ref.shape[1])], 0)

    return read


def sure_kernel(fast, scal_ref, sig_ref, ham_ref, hop_ref, less_ref, great_ref, flow_ref, *scratch):
    base = pl.program_id(0) * sig_ref.shape[3]
    solver = Solver(fast, rows_of(sig_ref), scal_ref, ham_ref, less_ref, great_ref, scratch, base)
    slabs = solver.slabs
    solver.start(hop_ref)
    solver.level(slabs - 1, True)

    def down(step, carry):
        slab = slabs - 2 - step
        solver.fold(slab + 1)
        solver.level(slab, False)
        return carry

    lax.fori_loop(0, slabs - 1, down, 0)
    flow_ref[0] = solver.flow()
    solver.first()

    def up(slab, carry):
        solver.up(slab)
        return carry

    lax.fori_loop(1, slabs, up, 0)


def transport(scalars, sigma, hamiltonian, coupling, fast=False):
    slabs, owners, _, count, depth = sigma.shape[:5]
    some = count if fast else 1
    vmem = pl.BlockSpec(memory_space=pltpu.VMEM)
    blocks = jax.ShapeDtypeStruct((count, slabs, 2, W, W), F32)
    out_spec = pl.BlockSpec((some, slabs, 2, W, W), lambda e: (e, 0, 0, 0, 0))
    less_new, great_new, flow = pl.pallas_call(
        functools.partial(sure_kernel, fast),
        grid=(count // some,),
        out_shape=(blocks, blocks, jax.ShapeDtypeStruct((count // some, 8, W), F32)),
        in_specs=[
            pl.BlockSpec(memory_space=pltpu.SMEM),
            pl.BlockSpec((slabs, owners, 2, some, depth, W), lambda e: (0, 0, 0, e, 0, 0)),
            vmem,
            vmem,
        ],
        out_specs=(out_spec, out_spec, pl.BlockSpec((1, 8, W), lambda e: (e, 0, 0))),
        scratch_shapes=Solver.scratch(some, slabs),
        compiler_params=pltpu.CompilerParams(vmem_limit_bytes=48 * 1024 * 1024),
        cost_estimate=pl.CostEstimate(flops=20_000_000_000, bytes_accessed=8_000_000, transcendentals=0),
    )(scalars, sigma, hamiltonian, coupling)
    return less_new, great_new, jnp.sum(flow, axis=0)


MESH = pl.DeviceIdType.MESH


def remote(source, target, send_sem, recv_sem, peer):
    return pltpu.make_async_remote_copy(
        src_ref=source, dst_ref=target, send_sem=send_sem, recv_sem=recv_sem,
        device_id=peer, device_id_type=MESH,
    )


def exchange_kernel(
    by, n_energy, n_mom,
    weight_ref, less_ref, great_ref, sigma_ref,
    pack, near_a, near_b, half_a, half_b, share, high, low, send_sem, recv_sem,
):
    place = lax.axis_index("energy")
    me = lax.axis_index("mom")
    count, slabs = less_ref.shape[:2]
    depth = W // n_mom
    after = lax.rem(me + 1, n_mom)
    before = lax.rem(me + n_mom - 1, n_mom)
    across = lax.rem(me + 2, n_mom)
    over = {"energy": lax.rem(place + by, n_energy)}
    under = {"energy": lax.rem(place - by + n_energy, n_energy)}
    wrapped_up = lax.div(place + by, n_energy)
    wrapped_down = 1 - lax.div(place - by + n_energy, n_energy)
    kept_up = (1 - wrapped_up).astype(F32)
    kept_down = (1 - wrapped_down).astype(F32)
    emission = weight_ref[0] * (1.0 / n_mom)
    absorption = weight_ref[1] * (1.0 / n_mom)

    barrier = pltpu.get_barrier_semaphore()
    for peer in ({"mom": after}, {"mom": before}, over, under):
        pl.semaphore_signal(barrier, inc=1, device_id=peer, device_id_type=MESH)

    def send(kind, chunk, source, target, peer):
        copy = remote(source, target, send_sem.at[kind, chunk], recv_sem.at[kind, chunk], peer)
        copy.start()
        return copy

    sent = {}
    rows = lax.broadcasted_iota(jnp.int32, (depth, W), 0)
    cols = lax.broadcasted_iota(jnp.int32, (depth, W), 1)
    order = range(slabs - 1, -1, -1)
    for c in order:
        for part in range(n_mom):
            span = slice(part * depth, (part + 1) * depth)
            upper = cols > rows + part * depth
            for kind, ref in enumerate((less_ref, great_ref)):
                pack[c, part, kind] = jnp.where(upper, ref[:, c, 0, span], ref[:, c, 1, span])
        if c == slabs - 1:
            pl.semaphore_wait(barrier, 4)
        sent[0, c] = send(0, c, pack.at[c, across, 0], near_a.at[c], {"mom": after})
        sent[1, c] = send(1, c, pack.at[c, across, 1], near_b.at[c], {"mom": before})
    for c in order:
        sent[0, c].wait_recv()
        pack[c, after, 0] = pack[c, after, 0] + near_a[c]
        sent[1, c].wait_recv()
        pack[c, before, 1] = pack[c, before, 1] + near_b[c]
        sent[2, c] = send(2, c, pack.at[c, after], half_a.at[c], {"mom": after})
        sent[3, c] = send(3, c, pack.at[c, before], half_b.at[c], {"mom": before})
    for c in order:
        sent[2, c].wait_recv()
        sent[3, c].wait_recv()
        share[c] = pack[c, me] + (half_a[c] + half_b[c])
        sent[4, c] = send(4, c, share.at[c], high.at[c], under)
        sent[5, c] = send(5, c, share.at[c], low.at[c], over)
    for c in order:
        sent[4, c].wait_recv()
        sent[5, c].wait_recv()
        for j in range(count):
            if j < count - 1:
                up = [high[c, kind, j + wrapped_up] for kind in range(2)]
            else:
                up = [high[c, kind, j] * kept_up for kind in range(2)]
            if j > 0:
                down = [low[c, kind, j - wrapped_down] for kind in range(2)]
            else:
                down = [low[c, kind, j] * kept_down for kind in range(2)]
            sigma_ref[c, 0, j] = emission * up[0] + absorption * down[0]
            sigma_ref[c, 1, j] = emission * down[1] + absorption * up[1]
    for copy in sent.values():
        copy.wait_send()


def exchange(by, n_energy, n_mom, weight, lesser, greater):
    count, slabs = lesser.shape[:2]
    depth = W // n_mom
    vmem = pl.BlockSpec(memory_space=pltpu.VMEM)
    half = pltpu.VMEM((slabs, count, depth, W), F32)
    whole = pltpu.VMEM((slabs, 2, count, depth, W), F32)
    return pl.pallas_call(
        functools.partial(exchange_kernel, by, n_energy, n_mom),
        out_shape=jax.ShapeDtypeStruct((slabs, 2, count, depth, W), F32),
        in_specs=[pl.BlockSpec(memory_space=pltpu.SMEM), vmem, vmem],
        out_specs=vmem,
        scratch_shapes=[
            pltpu.VMEM((slabs, n_mom, 2, count, depth, W), F32),
            half, half, whole, whole, whole, whole, whole,
            pltpu.SemaphoreType.DMA((6, slabs)),
            pltpu.SemaphoreType.DMA((6, slabs)),
        ],
        compiler_params=pltpu.CompilerParams(
            collective_id=by, has_side_effects=True, vmem_limit_bytes=32 * 1024 * 1024
        ),
    )(weight, lesser, greater)


def fast_kernel(
    n_mom, inner, outer,
    scal_ref, share_ref, ham_ref, hop_ref, less_ref, great_ref, total_ref,
    sigma, first, second, tile, partial, send_sem, recv_sem, sum_send, sum_recv, *scratch,
):
    solver = Solver(True, rows_of(sigma), scal_ref, ham_ref, less_ref, great_ref, scratch)
    slabs = solver.slabs
    place = lax.axis_index("energy")
    me = lax.axis_index("mom")
    after = lax.rem(me + 1, n_mom)
    before = lax.rem(me + n_mom - 1, n_mom)
    low = lax.rem(place, inner)
    high = lax.div(place, inner)
    slot = high * n_mom + me

    def outer_peer(step):
        other = lax.rem(slot + step, outer)
        return other, {"energy": lax.div(other, n_mom) * inner + low, "mom": lax.rem(other, n_mom)}

    def inner_peer(step):
        other = lax.rem(low + step, inner)
        return other, {"energy": high * inner + other, "mom": me}

    barrier = pltpu.get_barrier_semaphore()
    for step in range(1, outer):
        pl.semaphore_signal(barrier, inc=1, device_id=outer_peer(step)[1], device_id_type=MESH)
    for step in range(1, inner):
        pl.semaphore_signal(barrier, inc=1, device_id=inner_peer(step)[1], device_id_type=MESH)

    def near(slab):
        for kind, peer in ((0, after), (1, before)):
            yield remote(
                share_ref.at[slab], sigma.at[slab, me],
                send_sem.at[kind, slab], recv_sem.at[kind, slab], {"mom": peer},
            )

    def far(slab):
        for kind, owner, peer in ((0, before, after), (1, after, before)):
            part = sigma.at[slab, owner, kind]
            yield remote(
                part, part, send_sem.at[2 + kind, slab], recv_sem.at[2 + kind, slab], {"mom": peer}
            )

    def started(copies):
        for copy in copies:
            copy.start()

    def arrived(copies):
        for copy in copies:
            copy.wait_recv()

    rest = range(slabs - 2, -1, -1)
    solver.start(hop_ref)
    for slab in range(slabs):
        sigma[slab, me] = share_ref[slab]
    pl.semaphore_wait(barrier, outer + inner - 2)
    started(near(slabs - 1))
    arrived(near(slabs - 1))
    started(far(slabs - 1))
    for slab in rest:
        started(near(slab))
    arrived(far(slabs - 1))

    def midway():
        for slab in rest:
            arrived(near(slab))
            started(far(slab))

    solver.level(slabs - 1, True, midway)

    def down(step, carry):
        slab = slabs - 2 - step
        solver.fold(slab + 1)
        arrived(far(slab))
        solver.level(slab, False)
        return carry

    lax.fori_loop(0, slabs - 1, down, 0)

    def round_of(source, slots, size, own, peer, base):
        def copy(index, step):
            return remote(
                source, slots.at[index], sum_send.at[base + step], sum_recv.at[base + index], peer(step)[1]
            )

        def begin():
            for step in range(1, size):
                copy(own, step).start()
            slots[own] = source[...]

        def end():
            for step in range(1, size):
                copy(peer(step)[0], step).wait_recv()
            result = slots[0]
            for index in range(1, size):
                result = result + slots[index]
            for step in range(1, size):
                copy(own, step).wait_send()
            return result

        return begin, end

    begin_outer, end_outer = round_of(tile, first, outer, slot, outer_peer, 0)
    begin_inner, end_inner = round_of(partial, second, inner, low, inner_peer, outer)
    tile[...] = solver.flow()
    solver.first()
    begin_outer()
    solver.up(1)
    partial[...] = end_outer()
    solver.up(2)
    begin_inner()
    for slab in range(3, slabs):
        solver.up(slab)
    total_ref[...] = end_inner()
    for slab in range(slabs):
        for copies in (near(slab), far(slab)):
            for copy in copies:
                copy.wait_send()


def quick(n_energy, n_mom, scalars, share, hamiltonian, coupling, inner=8):
    slabs, _, count, depth = share.shape[:4]
    outer = n_energy // inner * n_mom
    vmem = pl.BlockSpec(memory_space=pltpu.VMEM)
    blocks = jax.ShapeDtypeStruct((count, slabs, 2, W, W), F32)
    return pl.pallas_call(
        functools.partial(fast_kernel, n_mom, inner, outer),
        out_shape=(blocks, blocks, jax.ShapeDtypeStruct((8, W), F32)),
        in_specs=[pl.BlockSpec(memory_space=pltpu.SMEM), vmem, vmem, vmem],
        out_specs=(vmem, vmem, vmem),
        scratch_shapes=[
            pltpu.VMEM((slabs, n_mom, 2, count, depth, W), F32),
            pltpu.VMEM((outer, 8, W), F32),
            pltpu.VMEM((inner, 8, W), F32),
            pltpu.VMEM((8, W), F32),
            pltpu.VMEM((8, W), F32),
            pltpu.SemaphoreType.DMA((4, slabs)),
            pltpu.SemaphoreType.DMA((4, slabs)),
            pltpu.SemaphoreType.DMA((outer + inner,)),
            pltpu.SemaphoreType.DMA((outer + inner,)),
        ]
        + Solver.scratch(count, slabs),
        compiler_params=pltpu.CompilerParams(
            collective_id=SMAX + 1, has_side_effects=True, vmem_limit_bytes=48 * 1024 * 1024
        ),
    )(scalars, share, hamiltonian, coupling)


def shards(lesser, greater, hamiltonian, coupling, shift, phonon_weight):
    n_energy = lax.axis_size("energy")
    n_mom = lax.axis_size("mom")
    here = lax.axis_index("energy")
    count = lesser.shape[0]
    total = count * n_energy
    branches = [functools.partial(exchange, k + 1, n_energy, n_mom) for k in range(SMAX)]
    share = lax.switch(shift[0] - 1, branches, phonon_weight, lesser[:, 0, 0], greater[:, 0, 0])
    grid = (jnp.arange(count) * n_energy + here).astype(F32)
    energy = (grid + 0.5) * (2.0 * band_edge / total) - band_edge
    scalars = jnp.stack(
        [
            energy,
            jax.nn.sigmoid((left_level - energy) / thermal),
            jax.nn.sigmoid((right_level - energy) / thermal),
        ]
    )
    ham, hop = hamiltonian[0], coupling[0]
    less_new, great_new, tile = quick(n_energy, n_mom, scalars, share, ham, hop)

    def again(share, less_new, great_new, flow):
        sigma = jnp.swapaxes(lax.all_gather(share, "mom", axis=0), 0, 1)
        less_new, great_new, tile = transport(scalars, sigma, ham, hop)
        return less_new, great_new, lax.psum(tile[0, 0], ("energy", "mom"))

    def keep(share, less_new, great_new, flow):
        return less_new, great_new, flow

    less_new, great_new, flow = lax.cond(
        tile[1, 0] > 0.5, again, keep, share, less_new, great_new, tile[0, 0]
    )
    current = flow * (2.0 * band_edge / total)
    return (less_new[:, None, None], great_new[:, None, None], current)


def solution(mesh):
    return jax.shard_map(
        shards,
        mesh=mesh,
        in_specs=(
            P(None, "energy", "mom", None, None, None, None),
            P(None, "energy", "mom", None, None, None, None),
            P("mom", None, None, None, None),
            P("mom", None, None, None),
            P(),
            P(),
        ),
        out_specs=(
            P(None, "energy", "mom", None, None, None, None),
            P(None, "energy", "mom", None, None, None, None),
            P(),
        ),
        check_vma=False,
    )
```

```python
import functools

import jax
import jax.numpy as jnp
from jax import lax
from jax.experimental import pallas as pl
from jax.experimental.pallas import tpu as pltpu
from jax.sharding import PartitionSpec as P

SMAX = 7
broaden = 0.2
contact_rate = 0.5
left_level = 0.3
right_level = -0.3
thermal = 0.1
band_edge = 2.0

W = 128
BF = jnp.bfloat16
F32 = jnp.float32
LEAST = 0.03


def store(ref, real, imag):
    for row, part in ((0, real), (W, imag)):
        high = part.astype(BF)
        ref[row : row + W, :W] = high
        ref[row : row + W, W:] = (part - high.astype(F32)).astype(BF)


def store_high(ref, real, imag):
    ref[:W, :W] = real.astype(BF)
    ref[W:, :W] = imag.astype(BF)


def unpacked(value, rows, cols):
    turned = value.T
    real = jnp.where(rows < cols, value, jnp.where(rows > cols, -turned, 0.0))
    imag = jnp.where(rows >= cols, value, turned)
    return real, imag


def product(left, right, dagger=False, high=False):
    if high:
        lhs = left[:, :W]
    else:
        whole = left[...]
        lhs = jnp.concatenate([whole, whole], 1)
    if dagger:
        up = right[:, :W]
        low = None if high else right[:, W:]
        rhs = up if high else jnp.concatenate([up, up, low, low], 1)
        dims = (((1,), (1,)), ((), ()))
    else:
        up = jnp.concatenate([right[:W, :W], right[W:, :W]], 1)
        if high:
            rhs = up
        else:
            low = jnp.concatenate([right[:W, W:], right[W:, W:]], 1)
            rhs = jnp.concatenate([up, up, low, low], 0)
        dims = (((1,), (0,)), ((), ()))
    full = lax.dot_general(lhs, rhs, dims, preferred_element_type=F32)
    if dagger:
        return full[:W, :W] + full[W:, W:], full[W:, :W] - full[:W, W:]
    return full[:W, :W] - full[W:, W:], full[:W, W:] + full[W:, :W]


FAST_LOW = 0.006
FAST_TOP = 0.4
FAST_GROW = 5
FAST_REFINE = 2
RESIDUAL = 1.0e-4


def schedule():
    lowest, steps = FAST_LOW, []
    for step in range(FAST_GROW):
        used = max(lowest, LEAST)
        a = 4.0 / (1.0 + used)
        b = a / (1.0 + used)
        lowest = min(lowest * (a - b * lowest), b * used)
        centre = 2.0 / (1.0 + lowest) if step == FAST_GROW - 1 else 1.0
        steps.append((a * centre, b * centre))
    return steps


class Solver:
    names = (
        "hop_f", "sys_f", "inv_f", "tmp_f", "inj_f", "gr_f", "t_f", "l_f", "full_f",
        "inv", "gl", "gr", "folded_r", "folded_l", "rho",
    )

    def __init__(self, fast, sigma, scal, ham, out, scratch, base=0):
        self.fast = fast
        self.sigma = sigma
        self.scal = lambda row, e: scal[row, base + e]
        self.ham = ham
        self.out = out
        for name, ref in zip(self.names, scratch, strict=True):
            setattr(self, name, ref)
        self.count = self.inv.shape[0]
        self.slabs = ham.shape[0]
        self.energies = range(self.count)
        self.rows = lax.broadcasted_iota(jnp.int32, (W, W), 0)
        self.cols = lax.broadcasted_iota(jnp.int32, (W, W), 1)
        self.eye = jnp.where(self.rows == self.cols, 1.0, 0.0).astype(F32)

    @classmethod
    def scratch(cls, count, slabs):
        form = (2 * W, 2 * W)
        blocks = (count, 2, W, W)
        few = pltpu.VMEM((count,) + form, BF)
        many = pltpu.VMEM((slabs, count) + form, BF)
        every = pltpu.VMEM((slabs,) + blocks, F32)
        own = pltpu.VMEM(blocks, F32)
        return [
            pltpu.VMEM(form, BF), few, few, few, few, many, many, many,
            pltpu.VMEM((2, count) + form, BF), own, every, every, own, own, pltpu.VMEM((8, W), F32),
        ]

    def start(self, hop):
        store(self.hop_f, hop[0].T, -hop[1].T)
        self.rho[...] = jnp.zeros((8, W), F32)

    def block(self, sigma, slab, kind, e):
        return unpacked(sigma(slab, kind, e), self.rows, self.cols)

    def grow_step(self, a, b):
        for e in self.energies:
            real, imag = product(self.inv_f.at[e], self.sys_f.at[e], high=True)
            store_high(self.tmp_f.at[e], real, imag)
        for e in self.energies:
            real, imag = product(self.tmp_f.at[e], self.inv_f.at[e], high=True)
            real = a * self.inv[e, 0] - b * real
            imag = a * self.inv[e, 1] - b * imag
            self.inv[e, 0] = real
            self.inv[e, 1] = imag
            store_high(self.inv_f.at[e], real, imag)

    def whole_form(self):
        for e in self.energies:
            store(self.inv_f.at[e], self.inv[e, 0], self.inv[e, 1])

    def refine_step(self):
        sizes = []
        for e in self.energies:
            real, imag = product(self.inv_f.at[e], self.sys_f.at[e])
            real = self.eye - real
            sizes.append(jnp.sum(real * real + imag * imag, axis=0, keepdims=True))
            store_high(self.tmp_f.at[e], real, -imag)
        for e in self.energies:
            real, imag = product(self.tmp_f.at[e], self.inv_f.at[e], high=True)
            real = self.inv[e, 0] + real
            imag = self.inv[e, 1] + imag
            self.inv[e, 0] = real
            self.inv[e, 1] = imag
            store(self.inv_f.at[e], real, imag)
        return sizes

    def invert(self, midway):
        norms = []
        for e in self.energies:
            real, imag = product(self.inv_f.at[e], self.sys_f.at[e], high=True)
            norms.append(jnp.sum(jnp.sqrt(real * real + imag * imag), axis=0, keepdims=True))
            if self.fast:
                store_high(self.tmp_f.at[e], real, imag)
        bound = 1.05 * jnp.max(functools.reduce(jnp.maximum, norms))
        if self.fast:
            steps = schedule()
            scale = 1.0 / (FAST_TOP * bound)
            first = steps[0][0] * scale
            second = steps[0][1] * scale * scale
            for e in self.energies:
                real, imag = product(self.tmp_f.at[e], self.inv_f.at[e], high=True)
                real = first * self.inv[e, 0] - second * real
                imag = first * self.inv[e, 1] - second * imag
                self.inv[e, 0] = real
                self.inv[e, 1] = imag
                store_high(self.inv_f.at[e], real, imag)
            for place, (a, b) in enumerate(steps[1:]):
                self.grow_step(a, b)
                if place == 1 and midway is not None:
                    midway()
            self.whole_form()
            for step in range(FAST_REFINE):
                sizes = self.refine_step()
            self.rho[0:1] = self.rho[0:1] + functools.reduce(jnp.add, sizes)
            return
        scale = 1.0 / bound
        for e in self.energies:
            real = self.inv[e, 0] * scale
            imag = self.inv[e, 1] * scale
            self.inv[e, 0] = real
            self.inv[e, 1] = imag
        self.whole_form()

        def grow(carry):
            lowest, done = carry
            used = jnp.maximum(lowest, LEAST)
            a = 4.0 / (1.0 + used)
            b = a / (1.0 + used)
            after = jnp.minimum(lowest * (a - b * lowest), b * used)
            for e in self.energies:
                real, imag = product(self.inv_f.at[e], self.sys_f.at[e])
                store(self.tmp_f.at[e], real, imag)
            for e in self.energies:
                real, imag = product(self.tmp_f.at[e], self.inv_f.at[e])
                real = a * self.inv[e, 0] - b * real
                imag = a * self.inv[e, 1] - b * imag
                self.inv[e, 0] = real
                self.inv[e, 1] = imag
                store(self.inv_f.at[e], real, imag)
            return after, done + 1

        lax.while_loop(
            lambda carry: jnp.logical_and(carry[0] < 0.9, carry[1] < 64),
            grow,
            (broaden * broaden * scale, jnp.int32(0)),
        )

        def refine(carry):
            sizes = [jnp.sum(size) for size in self.refine_step()]
            return functools.reduce(jnp.maximum, sizes), carry[1] + 1

        lax.while_loop(
            lambda carry: jnp.logical_and(carry[0] > 4.0e-6, carry[1] < 24),
            refine,
            (jnp.float32(1.0), jnp.int32(0)),
        )

    def level(self, slab, last, midway=None, sigma=None):
        sigma = self.sigma if sigma is None else sigma
        at_left = 0.0 if last else jnp.where(slab == 0, 1.0, 0.0)
        for e in self.energies:
            less = self.block(sigma, slab, 0, e)
            great = self.block(sigma, slab, 1, e)
            fill = self.scal(2, e) if last else at_left * self.scal(1, e)
            contact = contact_rate if last else at_left * contact_rate
            sys_r = self.scal(0, e) * self.eye - self.ham[slab, 0] - 0.5 * (great[0] - less[0])
            sys_i = (broaden + contact) * self.eye - self.ham[slab, 1] - 0.5 * (great[1] - less[1])
            inj_r = less[0]
            inj_i = less[1] + 2.0 * contact_rate * fill * self.eye
            if not last:
                sys_r = sys_r - self.folded_r[e, 0]
                sys_i = sys_i - self.folded_r[e, 1]
                inj_r = inj_r + self.folded_l[e, 0]
                inj_i = inj_i + self.folded_l[e, 1]
            store(self.sys_f.at[e], sys_r, sys_i)
            store(self.inj_f.at[e], inj_r, inj_i)
            back_r = sys_r.T
            back_i = -sys_i.T
            self.inv[e, 0] = back_r
            self.inv[e, 1] = back_i
            store_high(self.inv_f.at[e], back_r, back_i)
        self.invert(midway)
        for e in self.energies:
            self.gr[slab, e] = self.inv[e]
            self.gr_f[slab, e] = self.inv_f[e]
            real, imag = product(self.inv_f.at[e], self.inj_f.at[e])
            store(self.tmp_f.at[e], real, imag)
        for e in self.energies:
            real, imag = product(self.tmp_f.at[e], self.inv_f.at[e], dagger=True)
            self.gl[slab, e, 0] = real
            self.gl[slab, e, 1] = imag
            store(self.inj_f.at[e], real, imag)

    def fold(self, slab):
        for e in self.energies:
            real, imag = product(self.hop_f, self.gr_f.at[slab, e])
            store(self.t_f.at[slab, e], real, imag)
            real, imag = product(self.hop_f, self.inj_f.at[e])
            store(self.l_f.at[slab, e], real, imag)
        for e in self.energies:
            real, imag = product(self.t_f.at[slab, e], self.hop_f, dagger=True)
            self.folded_r[e, 0] = real
            self.folded_r[e, 1] = imag
            real, imag = product(self.l_f.at[slab, e], self.hop_f, dagger=True)
            self.folded_l[e, 0] = real
            self.folded_l[e, 1] = imag

    def flow(self):
        flow = jnp.zeros((1, W), F32)
        for e in self.energies:
            fill = self.scal(1, e)
            less = self.gl[0, e, 1]
            mixed = fill * (less + 2.0 * self.gr[0, e, 1]) + (1.0 - fill) * less
            flow = flow - jnp.sum(mixed * self.eye, axis=0, keepdims=True)
        flow = jnp.broadcast_to(jnp.sum(flow, axis=1, keepdims=True), (8, W))
        missed = jnp.broadcast_to(jnp.sum(self.rho[0:1], axis=1, keepdims=True), (8, W))
        missed = jnp.where(missed <= RESIDUAL, 0.0, 1.0)
        return jnp.where(lax.broadcasted_iota(jnp.int32, (8, W), 0) == 0, flow, missed)

    def finish(self, slab, e, green, less):
        great = (less[0] + green[0] - green[0].T, less[1] + green[1] + green[1].T)
        upper = self.rows < self.cols
        self.out[e, slab, 0] = jnp.where(upper, less[0], less[1])
        self.out[e, slab, 1] = jnp.where(upper, great[0], great[1])
        store(self.full_f.at[0, e], *green)
        store(self.full_f.at[1, e], *less)

    def first(self):
        for e in self.energies:
            self.finish(0, e, (self.gr[0, e, 0], self.gr[0, e, 1]), (self.gl[0, e, 0], self.gl[0, e, 1]))

    def up(self, slab):
        for e in self.energies:
            real, imag = product(self.gr_f.at[slab, e], self.hop_f, dagger=True)
            store(self.sys_f.at[e], real, imag)
        for e in self.energies:
            real, imag = product(self.sys_f.at[e], self.full_f.at[0, e])
            store(self.tmp_f.at[e], real, imag)
            real, imag = product(self.sys_f.at[e], self.full_f.at[1, e])
            store(self.inj_f.at[e], real, imag)
        for e in self.energies:
            real, imag = product(self.tmp_f.at[e], self.t_f.at[slab, e])
            green = (self.gr[slab, e, 0] + real, self.gr[slab, e, 1] + imag)
            cross = product(self.tmp_f.at[e], self.l_f.at[slab, e])
            real, imag = product(self.inj_f.at[e], self.sys_f.at[e], dagger=True)
            less = (
                self.gl[slab, e, 0] + real + cross[0] - cross[0].T,
                self.gl[slab, e, 1] + imag + cross[1] + cross[1].T,
            )
            self.finish(slab, e, green, less)


def rows_of(sigma_ref):
    def read(slab, kind, e):
        return jnp.concatenate([sigma_ref[slab, owner, kind, e] for owner in range(sigma_ref.shape[1])], 0)

    return read


def sure_kernel(fast, scal_ref, sig_ref, ham_ref, hop_ref, out_ref, flow_ref, *scratch):
    base = pl.program_id(0) * sig_ref.shape[3]
    solver = Solver(fast, rows_of(sig_ref), scal_ref, ham_ref, out_ref, scratch, base)
    slabs = solver.slabs
    solver.start(hop_ref)
    solver.level(slabs - 1, True)

    def down(step, carry):
        slab = slabs - 2 - step
        solver.fold(slab + 1)
        solver.level(slab, False)
        return carry

    lax.fori_loop(0, slabs - 1, down, 0)
    flow_ref[0] = solver.flow()
    solver.first()

    def up(slab, carry):
        solver.up(slab)
        return carry

    lax.fori_loop(1, slabs, up, 0)


def transport(scalars, sigma, hamiltonian, coupling, fast=False):
    slabs, owners, _, count, depth = sigma.shape[:5]
    some = count if fast else 1
    vmem = pl.BlockSpec(memory_space=pltpu.VMEM)
    blocks = jax.ShapeDtypeStruct((count, slabs, 2, W, W), F32)
    out_spec = pl.BlockSpec((some, slabs, 2, W, W), lambda e: (e, 0, 0, 0, 0))
    packed, flow = pl.pallas_call(
        functools.partial(sure_kernel, fast),
        grid=(count // some,),
        out_shape=(blocks, jax.ShapeDtypeStruct((count // some, 8, W), F32)),
        in_specs=[
            pl.BlockSpec(memory_space=pltpu.SMEM),
            pl.BlockSpec((slabs, owners, 2, some, depth, W), lambda e: (0, 0, 0, e, 0, 0)),
            vmem,
            vmem,
        ],
        out_specs=(out_spec, pl.BlockSpec((1, 8, W), lambda e: (e, 0, 0))),
        scratch_shapes=Solver.scratch(some, slabs),
        compiler_params=pltpu.CompilerParams(vmem_limit_bytes=(44 if fast else 16) * 1024 * 1024),
        cost_estimate=pl.CostEstimate(flops=20_000_000_000, bytes_accessed=8_000_000, transcendentals=0),
    )(scalars, sigma, hamiltonian, coupling)
    return packed, jnp.sum(flow, axis=0)


def spread_kernel(packed_ref, less_ref, great_ref):
    rows = lax.broadcasted_iota(jnp.int32, (W, W), 0)
    cols = lax.broadcasted_iota(jnp.int32, (W, W), 1)
    for slab in range(packed_ref.shape[1]):
        for kind, ref in enumerate((less_ref, great_ref)):
            real, imag = unpacked(packed_ref[0, slab, kind], rows, cols)
            ref[0, slab, 0] = real
            ref[0, slab, 1] = imag


def spread(packed):
    spec = pl.BlockSpec((1,) + packed.shape[1:], lambda e: (e, 0, 0, 0, 0))
    return pl.pallas_call(
        spread_kernel,
        grid=(packed.shape[0],),
        out_shape=(jax.ShapeDtypeStruct(packed.shape, F32),) * 2,
        in_specs=[spec],
        out_specs=(spec, spec),
        compiler_params=pltpu.CompilerParams(vmem_limit_bytes=16 * 1024 * 1024),
    )(packed)


MESH = pl.DeviceIdType.MESH
GATHERED = 2


def remote(source, target, send_sem, recv_sem, peer):
    return pltpu.make_async_remote_copy(
        src_ref=source, dst_ref=target, send_sem=send_sem, recv_sem=recv_sem,
        device_id=peer, device_id_type=MESH,
    )


def exchange_kernel(
    by, n_energy, n_mom,
    weight_ref, less_ref, great_ref, sigma_ref,
    pack, near_a, near_b, half_a, half_b, share, high, low, send_sem, recv_sem,
):
    place = lax.axis_index("energy")
    me = lax.axis_index("mom")
    count, slabs = less_ref.shape[:2]
    depth = W // n_mom
    after = lax.rem(me + 1, n_mom)
    before = lax.rem(me + n_mom - 1, n_mom)
    across = lax.rem(me + 2, n_mom)
    over = {"energy": lax.rem(place + by, n_energy)}
    under = {"energy": lax.rem(place - by + n_energy, n_energy)}
    wrapped_up = lax.div(place + by, n_energy)
    wrapped_down = 1 - lax.div(place - by + n_energy, n_energy)
    kept_up = (1 - wrapped_up).astype(F32)
    kept_down = (1 - wrapped_down).astype(F32)
    emission = weight_ref[0] * (1.0 / n_mom)
    absorption = weight_ref[1] * (1.0 / n_mom)

    barrier = pltpu.get_barrier_semaphore()
    for peer in ({"mom": after}, {"mom": before}, over, under):
        pl.semaphore_signal(barrier, inc=1, device_id=peer, device_id_type=MESH)

    def send(kind, chunk, source, target, peer):
        copy = remote(source, target, send_sem.at[kind, chunk], recv_sem.at[kind, chunk], peer)
        copy.start()
        return copy

    sent = {}

    def pass_on(c):
        sent[6, c].wait_recv()
        part = sigma_ref.at[c, before, 0]
        sent[8, c] = send(8, c, part, part, {"mom": after})
        sent[7, c].wait_recv()
        part = sigma_ref.at[c, after, 1]
        sent[9, c] = send(9, c, part, part, {"mom": before})

    rows = lax.broadcasted_iota(jnp.int32, (depth, W), 0)
    cols = lax.broadcasted_iota(jnp.int32, (depth, W), 1)
    order = range(slabs - 1, -1, -1)
    for c in order:
        for part in range(n_mom):
            span = slice(part * depth, (part + 1) * depth)
            upper = cols > rows + part * depth
            for kind, ref in enumerate((less_ref, great_ref)):
                pack[c, part, kind] = jnp.where(upper, ref[:, c, 0, span], ref[:, c, 1, span])
        if c == slabs - 1:
            pl.semaphore_wait(barrier, 4)
        sent[0, c] = send(0, c, pack.at[c, across, 0], near_a.at[c], {"mom": after})
        sent[1, c] = send(1, c, pack.at[c, across, 1], near_b.at[c], {"mom": before})
    for c in order:
        sent[0, c].wait_recv()
        pack[c, after, 0] = pack[c, after, 0] + near_a[c]
        sent[1, c].wait_recv()
        pack[c, before, 1] = pack[c, before, 1] + near_b[c]
        sent[2, c] = send(2, c, pack.at[c, after], half_a.at[c], {"mom": after})
        sent[3, c] = send(3, c, pack.at[c, before], half_b.at[c], {"mom": before})
    for c in order:
        sent[2, c].wait_recv()
        sent[3, c].wait_recv()
        share[c] = pack[c, me] + (half_a[c] + half_b[c])
        sent[4, c] = send(4, c, share.at[c], high.at[c], under)
        sent[5, c] = send(5, c, share.at[c], low.at[c], over)
    for c in order:
        sent[4, c].wait_recv()
        sent[5, c].wait_recv()
        for j in range(count):
            if j < count - 1:
                up = [high[c, kind, j + wrapped_up] for kind in range(2)]
            else:
                up = [high[c, kind, j] * kept_up for kind in range(2)]
            if j > 0:
                down = [low[c, kind, j - wrapped_down] for kind in range(2)]
            else:
                down = [low[c, kind, j] * kept_down for kind in range(2)]
            sigma_ref[c, me, 0, j] = emission * up[0] + absorption * down[0]
            sigma_ref[c, me, 1, j] = emission * down[1] + absorption * up[1]
        if c >= slabs - GATHERED:
            mine = sigma_ref.at[c, me]
            sent[6, c] = send(6, c, mine, mine, {"mom": after})
            sent[7, c] = send(7, c, mine, mine, {"mom": before})
        if c + 1 < slabs and c + 1 >= slabs - GATHERED:
            pass_on(c + 1)
    for c in order:
        if (8, c) in sent:
            sent[8, c].wait_recv()
            sent[9, c].wait_recv()
    for copy in sent.values():
        copy.wait_send()


def exchange(by, n_energy, n_mom, weight, lesser, greater):
    count, slabs = lesser.shape[:2]
    depth = W // n_mom
    vmem = pl.BlockSpec(memory_space=pltpu.VMEM)
    half = pltpu.VMEM((slabs, count, depth, W), F32)
    whole = pltpu.VMEM((slabs, 2, count, depth, W), F32)
    return pl.pallas_call(
        functools.partial(exchange_kernel, by, n_energy, n_mom),
        out_shape=jax.ShapeDtypeStruct((slabs, n_mom, 2, count, depth, W), F32),
        in_specs=[pl.BlockSpec(memory_space=pltpu.SMEM), vmem, vmem],
        out_specs=vmem,
        scratch_shapes=[
            pltpu.VMEM((slabs, n_mom, 2, count, depth, W), F32),
            half, half, whole, whole, whole, whole, whole,
            pltpu.SemaphoreType.DMA((10, slabs)),
            pltpu.SemaphoreType.DMA((10, slabs)),
        ],
        compiler_params=pltpu.CompilerParams(
            collective_id=by, has_side_effects=True, vmem_limit_bytes=32 * 1024 * 1024
        ),
    )(weight, lesser, greater)


def fast_kernel(
    n_mom, inner, outer,
    scal_ref, share_ref, ham_ref, hop_ref, out_ref, total_ref,
    sigma, first, second, tile, partial, send_sem, recv_sem, sum_send, sum_recv, *scratch,
):
    solver = Solver(True, rows_of(sigma), scal_ref, ham_ref, out_ref, scratch)
    slabs = solver.slabs
    place = lax.axis_index("energy")
    me = lax.axis_index("mom")
    after = lax.rem(me + 1, n_mom)
    before = lax.rem(me + n_mom - 1, n_mom)
    low = lax.rem(place, inner)
    high = lax.div(place, inner)
    slot = high * n_mom + me

    def outer_peer(step):
        other = lax.rem(slot + step, outer)
        return other, {"energy": lax.div(other, n_mom) * inner + low, "mom": lax.rem(other, n_mom)}

    def inner_peer(step):
        other = lax.rem(low + step, inner)
        return other, {"energy": high * inner + other, "mom": me}

    barrier = pltpu.get_barrier_semaphore()
    for step in range(1, outer):
        pl.semaphore_signal(barrier, inc=1, device_id=outer_peer(step)[1], device_id_type=MESH)
    for step in range(1, inner):
        pl.semaphore_signal(barrier, inc=1, device_id=inner_peer(step)[1], device_id_type=MESH)

    def near(slab):
        for kind, peer in ((0, after), (1, before)):
            yield remote(
                share_ref.at[slab, me], sigma.at[slab, me],
                send_sem.at[kind, slab], recv_sem.at[kind, slab], {"mom": peer},
            )

    def far(slab):
        for kind, owner, peer in ((0, before, after), (1, after, before)):
            part = sigma.at[slab, owner, kind]
            yield remote(
                part, part, send_sem.at[2 + kind, slab], recv_sem.at[2 + kind, slab], {"mom": peer}
            )

    def started(copies):
        for copy in copies:
            copy.start()

    def arrived(copies):
        for copy in copies:
            copy.wait_recv()

    rest = range(slabs - GATHERED - 1, -1, -1)

    def share_rest():
        pl.semaphore_wait(barrier, outer + inner - 2)
        for slab in range(slabs - GATHERED, slabs - 1):
            sigma[slab] = share_ref[slab]
        for slab in rest:
            started(near(slab))
            sigma[slab, me] = share_ref[slab, me]

    solver.start(hop_ref)
    solver.level(slabs - 1, True, share_rest, rows_of(share_ref))

    def down(step, carry):
        slab = slabs - 2 - step

        def pass_on():
            @pl.when(step == 0)
            def _():
                for other in rest:
                    arrived(near(other))
                    started(far(other))

        solver.fold(slab + 1)

        @pl.when(slab < slabs - GATHERED)
        def _():
            arrived(far(slab))

        solver.level(slab, False, pass_on)
        return carry

    lax.fori_loop(0, slabs - 1, down, 0)

    def round_of(source, slots, size, own, peer, base):
        def copy(index, step):
            return remote(
                source, slots.at[index], sum_send.at[base + step], sum_recv.at[base + index], peer(step)[1]
            )

        def begin():
            for step in range(1, size):
                copy(own, step).start()
            slots[own] = source[...]

        def end():
            for step in range(1, size):
                copy(peer(step)[0], step).wait_recv()
            result = slots[0]
            for index in range(1, size):
                result = result + slots[index]
            for step in range(1, size):
                copy(own, step).wait_send()
            return result

        return begin, end

    begin_outer, end_outer = round_of(tile, first, outer, slot, outer_peer, 0)
    begin_inner, end_inner = round_of(partial, second, inner, low, inner_peer, outer)
    tile[...] = solver.flow()
    solver.first()
    begin_outer()
    solver.up(1)
    partial[...] = end_outer()
    solver.up(2)
    begin_inner()
    for slab in range(3, slabs):
        solver.up(slab)
    total_ref[...] = end_inner()
    for slab in rest:
        for copies in (near(slab), far(slab)):
            for copy in copies:
                copy.wait_send()


def quick(n_energy, n_mom, scalars, share, hamiltonian, coupling, inner=8):
    slabs, _, _, count, depth = share.shape[:5]
    outer = n_energy // inner * n_mom
    vmem = pl.BlockSpec(memory_space=pltpu.VMEM)
    blocks = jax.ShapeDtypeStruct((count, slabs, 2, W, W), F32)
    return pl.pallas_call(
        functools.partial(fast_kernel, n_mom, inner, outer),
        out_shape=(blocks, jax.ShapeDtypeStruct((8, W), F32)),
        in_specs=[pl.BlockSpec(memory_space=pltpu.SMEM), vmem, vmem, vmem],
        out_specs=(vmem, vmem),
        scratch_shapes=[
            pltpu.VMEM((slabs, n_mom, 2, count, depth, W), F32),
            pltpu.VMEM((outer, 8, W), F32),
            pltpu.VMEM((inner, 8, W), F32),
            pltpu.VMEM((8, W), F32),
            pltpu.VMEM((8, W), F32),
            pltpu.SemaphoreType.DMA((4, slabs)),
            pltpu.SemaphoreType.DMA((4, slabs)),
            pltpu.SemaphoreType.DMA((outer + inner,)),
            pltpu.SemaphoreType.DMA((outer + inner,)),
        ]
        + Solver.scratch(count, slabs),
        compiler_params=pltpu.CompilerParams(
            collective_id=SMAX + 1, has_side_effects=True, vmem_limit_bytes=26 * 1024 * 1024
        ),
    )(scalars, share, hamiltonian, coupling)


def moved(array, axis, by):
    size = lax.axis_size(axis)
    return lax.ppermute(array, axis, [(i, (i + by) % size) for i in range(size)]) if by else array


def shards(lesser, greater, hamiltonian, coupling, shift, phonon_weight):
    n_energy = lax.axis_size("energy")
    n_mom = lax.axis_size("mom")
    here = lax.axis_index("energy")
    count = lesser.shape[0]
    total = count * n_energy
    branches = [functools.partial(exchange, k + 1, n_energy, n_mom) for k in range(SMAX)]
    share = lax.switch(shift[0] - 1, branches, phonon_weight, lesser[:, 0, 0], greater[:, 0, 0])
    grid = (jnp.arange(count) * n_energy + here).astype(F32)
    energy = (grid + 0.5) * (2.0 * band_edge / total) - band_edge
    scalars = jnp.stack(
        [
            energy,
            jax.nn.sigmoid((left_level - energy) / thermal),
            jax.nn.sigmoid((right_level - energy) / thermal),
        ]
    )
    ham, hop = hamiltonian[0], coupling[0]
    packed, tile = quick(n_energy, n_mom, scalars, share, ham, hop)

    def again(share, packed, tile):
        mine = share[:, lax.axis_index("mom")]
        parts = jnp.stack([moved(mine, "mom", k) for k in range(n_mom)], 1)
        owners = (lax.axis_index("mom") - jnp.arange(n_mom)) % n_mom
        sigma = jnp.zeros_like(parts).at[:, owners].set(parts)
        packed, tile = transport(scalars, sigma, ham, hop)
        flow = tile[0, 0]
        for axis, size in (("mom", n_mom), ("energy", n_energy)):
            by = 1
            while by < size:
                flow = flow + lax.ppermute(flow, axis, [(i, i ^ by) for i in range(size)])
                by = 2 * by
        return (*spread(packed), flow)

    def keep(share, packed, tile):
        return (*spread(packed), tile[0, 0])

    less_new, great_new, flow = lax.cond(tile[1, 0] > 0.5, again, keep, share, packed, tile)
    current = flow * (2.0 * band_edge / total)
    return (less_new[:, None, None], great_new[:, None, None], current)


def solution(mesh):
    return jax.shard_map(
        shards,
        mesh=mesh,
        in_specs=(
            P(None, "energy", "mom", None, None, None, None),
            P(None, "energy", "mom", None, None, None, None),
            P("mom", None, None, None, None),
            P("mom", None, None, None),
            P(),
            P(),
        ),
        out_specs=(
            P(None, "energy", "mom", None, None, None, None),
            P(None, "energy", "mom", None, None, None, None),
            P(),
        ),
        check_vma=False,
    )
```

```python
import functools

import jax
import jax.numpy as jnp
from jax import lax
from jax.experimental import pallas as pl
from jax.experimental.pallas import tpu as pltpu
from jax.sharding import PartitionSpec as P

SMAX = 7
POINTS = 128
broaden = 0.2
contact_rate = 0.5
left_level = 0.3
right_level = -0.3
thermal = 0.1
band_edge = 2.0

W = 128
BF = jnp.bfloat16
F32 = jnp.float32
LEAST = 0.03


def store(ref, real, imag):
    for row, part in ((0, real), (W, imag)):
        high = part.astype(BF)
        ref[row : row + W, :W] = high
        ref[row : row + W, W:] = (part - high.astype(F32)).astype(BF)


def store_high(ref, real, imag):
    ref[:W, :W] = real.astype(BF)
    ref[W:, :W] = imag.astype(BF)


def unpacked(value, rows, cols):
    turned = value.T
    real = jnp.where(rows < cols, value, jnp.where(rows > cols, -turned, 0.0))
    imag = jnp.where(rows >= cols, value, turned)
    return real, imag


def product(left, right, dagger=False, high=False):
    if dagger:
        up = right[:, :W]
        dims = (((1,), (1,)), ((), ()))
    else:
        up = jnp.concatenate([right[:W, :W], right[W:, :W]], 1)
        dims = (((1,), (0,)), ((), ()))
    if high:
        lhs, rhs = left[:, :W], up
    else:
        lhs, rhs = left[...], jnp.concatenate([up, up], 1 if dagger else 0)
    full = lax.dot_general(lhs, rhs, dims, preferred_element_type=F32)
    if dagger:
        real, imag = full[:W, :W] + full[W:, W:], full[W:, :W] - full[:W, W:]
    else:
        real, imag = full[:W, :W] - full[W:, W:], full[:W, W:] + full[W:, :W]
    if high:
        return real, imag
    lhs = jnp.concatenate([left[:W, :W], left[W:, :W]], 1)
    low_r, low_i = right[:W, W:], right[W:, W:]
    rhs = jnp.concatenate([jnp.concatenate([low_r, low_i], 1), jnp.concatenate([-low_i, low_r], 1)], 0)
    rest = lax.dot_general(lhs, rhs, dims, preferred_element_type=F32)
    return real + rest[:, :W], imag + rest[:, W:]


FAST_LOW = 0.006
FAST_TOP = 0.4
FAST_GROW = 5
FAST_REFINE = 2
RESIDUAL = 1.0e-4


def schedule():
    lowest, steps = FAST_LOW, []
    for step in range(FAST_GROW):
        used = max(lowest, LEAST)
        a = 4.0 / (1.0 + used)
        b = a / (1.0 + used)
        lowest = min(lowest * (a - b * lowest), b * used)
        centre = 2.0 / (1.0 + lowest) if step == FAST_GROW - 1 else 1.0
        steps.append((a * centre, b * centre))
    return steps


class Solver:
    names = (
        "hop_f", "sys_f", "inv_f", "tmp_f", "inj_f", "gr_f", "t_f", "l_f", "full_f",
        "inv", "gl", "gr", "folded_r", "folded_l", "rho",
    )

    def __init__(self, fast, sigma, scal, ham, out, scratch, base=0):
        self.fast = fast
        self.sigma = sigma
        self.scal = lambda row, e: scal[row, base + e]
        self.ham = ham
        self.out = out
        for name, ref in zip(self.names, scratch, strict=True):
            setattr(self, name, ref)
        self.count = self.inv.shape[0]
        self.weight = 2.0 * band_edge / POINTS
        self.slabs = ham.shape[0]
        self.energies = range(self.count)
        self.rows = lax.broadcasted_iota(jnp.int32, (W, W), 0)
        self.cols = lax.broadcasted_iota(jnp.int32, (W, W), 1)
        self.eye = jnp.where(self.rows == self.cols, 1.0, 0.0).astype(F32)

    @classmethod
    def scratch(cls, count, slabs):
        form = (2 * W, 2 * W)
        blocks = (count, 2, W, W)
        few = pltpu.VMEM((count,) + form, BF)
        many = pltpu.VMEM((slabs, count) + form, BF)
        every = pltpu.VMEM((slabs,) + blocks, F32)
        own = pltpu.VMEM(blocks, F32)
        return [
            pltpu.VMEM(form, BF), few, few, few, few, many, many, many,
            pltpu.VMEM((2, count) + form, BF), own, every, every, own, own, pltpu.VMEM((8, W), F32),
        ]

    def start(self, hop):
        store(self.hop_f, hop[0].T, -hop[1].T)
        self.rho[...] = jnp.zeros((8, W), F32)

    def block(self, sigma, slab, kind, e):
        return unpacked(sigma(slab, kind, e), self.rows, self.cols)

    def grow_step(self, a, b):
        for e in self.energies:
            real, imag = product(self.inv_f.at[e], self.sys_f.at[e], high=True)
            store_high(self.tmp_f.at[e], real, imag)
        for e in self.energies:
            real, imag = product(self.tmp_f.at[e], self.inv_f.at[e], high=True)
            real = a * self.inv[e, 0] - b * real
            imag = a * self.inv[e, 1] - b * imag
            self.inv[e, 0] = real
            self.inv[e, 1] = imag
            store_high(self.inv_f.at[e], real, imag)

    def whole_form(self):
        for e in self.energies:
            store(self.inv_f.at[e], self.inv[e, 0], self.inv[e, 1])

    def refine_step(self):
        sizes = []
        for e in self.energies:
            real, imag = product(self.inv_f.at[e], self.sys_f.at[e])
            real = self.eye - real
            sizes.append(jnp.sum(real * real + imag * imag, axis=0, keepdims=True))
            store_high(self.tmp_f.at[e], real, -imag)
        for e in self.energies:
            real, imag = product(self.tmp_f.at[e], self.inv_f.at[e], high=True)
            real = self.inv[e, 0] + real
            imag = self.inv[e, 1] + imag
            self.inv[e, 0] = real
            self.inv[e, 1] = imag
            store(self.inv_f.at[e], real, imag)
        return sizes

    def invert(self, midway):
        norms = []
        for e in self.energies:
            real, imag = product(self.inv_f.at[e], self.sys_f.at[e], high=True)
            norms.append(jnp.sum(jnp.sqrt(real * real + imag * imag), axis=0, keepdims=True))
            if self.fast:
                store_high(self.tmp_f.at[e], real, imag)
        bound = 1.05 * jnp.max(functools.reduce(jnp.maximum, norms))
        if self.fast:
            steps = schedule()
            scale = 1.0 / (FAST_TOP * bound)
            first = steps[0][0] * scale
            second = steps[0][1] * scale * scale
            for e in self.energies:
                real, imag = product(self.tmp_f.at[e], self.inv_f.at[e], high=True)
                real = first * self.inv[e, 0] - second * real
                imag = first * self.inv[e, 1] - second * imag
                self.inv[e, 0] = real
                self.inv[e, 1] = imag
                store_high(self.inv_f.at[e], real, imag)
            for place, (a, b) in enumerate(steps[1:]):
                self.grow_step(a, b)
                if place == 1 and midway is not None:
                    midway()
            self.whole_form()
            for step in range(FAST_REFINE):
                sizes = self.refine_step()
            self.rho[0:1] = self.rho[0:1] + functools.reduce(jnp.add, sizes)
            return
        scale = 1.0 / bound
        for e in self.energies:
            real = self.inv[e, 0] * scale
            imag = self.inv[e, 1] * scale
            self.inv[e, 0] = real
            self.inv[e, 1] = imag
        self.whole_form()

        def grow(carry):
            lowest, done = carry
            used = jnp.maximum(lowest, LEAST)
            a = 4.0 / (1.0 + used)
            b = a / (1.0 + used)
            after = jnp.minimum(lowest * (a - b * lowest), b * used)
            for e in self.energies:
                real, imag = product(self.inv_f.at[e], self.sys_f.at[e])
                store(self.tmp_f.at[e], real, imag)
            for e in self.energies:
                real, imag = product(self.tmp_f.at[e], self.inv_f.at[e])
                real = a * self.inv[e, 0] - b * real
                imag = a * self.inv[e, 1] - b * imag
                self.inv[e, 0] = real
                self.inv[e, 1] = imag
                store(self.inv_f.at[e], real, imag)
            return after, done + 1

        lax.while_loop(
            lambda carry: jnp.logical_and(carry[0] < 0.9, carry[1] < 64),
            grow,
            (broaden * broaden * scale, jnp.int32(0)),
        )

        def refine(carry):
            sizes = [jnp.sum(size) for size in self.refine_step()]
            return functools.reduce(jnp.maximum, sizes), carry[1] + 1

        lax.while_loop(
            lambda carry: jnp.logical_and(carry[0] > 4.0e-6, carry[1] < 24),
            refine,
            (jnp.float32(1.0), jnp.int32(0)),
        )

    def level(self, slab, last, midway=None, sigma=None):
        sigma = self.sigma if sigma is None else sigma
        at_left = 0.0 if last else jnp.where(slab == 0, 1.0, 0.0)
        for e in self.energies:
            less = self.block(sigma, slab, 0, e)
            great = self.block(sigma, slab, 1, e)
            fill = self.scal(2, e) if last else at_left * self.scal(1, e)
            contact = contact_rate if last else at_left * contact_rate
            sys_r = self.scal(0, e) * self.eye - self.ham[slab, 0] - 0.5 * (great[0] - less[0])
            sys_i = (broaden + contact) * self.eye - self.ham[slab, 1] - 0.5 * (great[1] - less[1])
            inj_r = less[0]
            inj_i = less[1] + 2.0 * contact_rate * fill * self.eye
            if not last:
                sys_r = sys_r - self.folded_r[e, 0]
                sys_i = sys_i - self.folded_r[e, 1]
                inj_r = inj_r + self.folded_l[e, 0]
                inj_i = inj_i + self.folded_l[e, 1]
            store(self.sys_f.at[e], sys_r, sys_i)
            store(self.inj_f.at[e], inj_r, inj_i)
            back_r = sys_r.T
            back_i = -sys_i.T
            self.inv[e, 0] = back_r
            self.inv[e, 1] = back_i
            store_high(self.inv_f.at[e], back_r, back_i)
        self.invert(midway)
        for e in self.energies:
            self.gr[slab, e] = self.inv[e]
            self.gr_f[slab, e] = self.inv_f[e]
            real, imag = product(self.inv_f.at[e], self.inj_f.at[e])
            store(self.tmp_f.at[e], real, imag)
        for e in self.energies:
            real, imag = product(self.tmp_f.at[e], self.inv_f.at[e], dagger=True)
            self.gl[slab, e, 0] = real
            self.gl[slab, e, 1] = imag
            store(self.inj_f.at[e], real, imag)

    def fold(self, slab):
        for e in self.energies:
            real, imag = product(self.hop_f, self.gr_f.at[slab, e])
            store(self.t_f.at[slab, e], real, imag)
            real, imag = product(self.hop_f, self.inj_f.at[e])
            store(self.l_f.at[slab, e], real, imag)
        for e in self.energies:
            real, imag = product(self.t_f.at[slab, e], self.hop_f, dagger=True)
            self.folded_r[e, 0] = real
            self.folded_r[e, 1] = imag
            real, imag = product(self.l_f.at[slab, e], self.hop_f, dagger=True)
            self.folded_l[e, 0] = real
            self.folded_l[e, 1] = imag

    def flow(self):
        flow = jnp.zeros((1, W), F32)
        for e in self.energies:
            fill = self.scal(1, e)
            less = self.gl[0, e, 1]
            mixed = fill * (less + 2.0 * self.gr[0, e, 1]) + (1.0 - fill) * less
            flow = flow - jnp.sum(mixed * self.eye, axis=0, keepdims=True)
        flow = jnp.broadcast_to(jnp.sum(flow, axis=1, keepdims=True) * self.weight, (8, W))
        missed = jnp.broadcast_to(jnp.sum(self.rho[0:1], axis=1, keepdims=True), (8, W))
        missed = jnp.where(missed <= RESIDUAL, 0.0, 1.0)
        return jnp.where(lax.broadcasted_iota(jnp.int32, (8, W), 0) == 0, flow, missed)

    def finish(self, slab, e, green, less):
        great = (less[0] + green[0] - green[0].T, less[1] + green[1] + green[1].T)
        upper = self.rows < self.cols
        self.out[e, slab, 0] = jnp.where(upper, less[0], less[1])
        self.out[e, slab, 1] = jnp.where(upper, great[0], great[1])
        store(self.full_f.at[0, e], *green)
        store(self.full_f.at[1, e], *less)

    def first(self):
        for e in self.energies:
            self.finish(0, e, (self.gr[0, e, 0], self.gr[0, e, 1]), (self.gl[0, e, 0], self.gl[0, e, 1]))

    def up(self, slab):
        for e in self.energies:
            real, imag = product(self.gr_f.at[slab, e], self.hop_f, dagger=True)
            store(self.sys_f.at[e], real, imag)
        for e in self.energies:
            real, imag = product(self.sys_f.at[e], self.full_f.at[0, e])
            store(self.tmp_f.at[e], real, imag)
            real, imag = product(self.sys_f.at[e], self.full_f.at[1, e])
            store(self.inj_f.at[e], real, imag)
        for e in self.energies:
            real, imag = product(self.tmp_f.at[e], self.t_f.at[slab, e])
            green = (self.gr[slab, e, 0] + real, self.gr[slab, e, 1] + imag)
            cross = product(self.tmp_f.at[e], self.l_f.at[slab, e])
            real, imag = product(self.inj_f.at[e], self.sys_f.at[e], dagger=True)
            less = (
                self.gl[slab, e, 0] + real + cross[0] - cross[0].T,
                self.gl[slab, e, 1] + imag + cross[1] + cross[1].T,
            )
            self.finish(slab, e, green, less)


def rows_of(sigma_ref):
    def read(slab, kind, e):
        return jnp.concatenate([sigma_ref[slab, owner, kind, e] for owner in range(sigma_ref.shape[1])], 0)

    return read


def sure_kernel(fast, scal_ref, sig_ref, ham_ref, hop_ref, out_ref, flow_ref, *scratch):
    base = pl.program_id(0) * sig_ref.shape[3]
    solver = Solver(fast, rows_of(sig_ref), scal_ref, ham_ref, out_ref, scratch, base)
    slabs = solver.slabs
    solver.start(hop_ref)
    solver.level(slabs - 1, True)

    def down(step, carry):
        slab = slabs - 2 - step
        solver.fold(slab + 1)
        solver.level(slab, False)
        return carry

    lax.fori_loop(0, slabs - 1, down, 0)
    flow_ref[0] = solver.flow()
    solver.first()

    def up(slab, carry):
        solver.up(slab)
        return carry

    lax.fori_loop(1, slabs, up, 0)


def transport(scalars, sigma, hamiltonian, coupling, fast=False):
    slabs, owners, _, count, depth = sigma.shape[:5]
    some = count if fast else 1
    vmem = pl.BlockSpec(memory_space=pltpu.VMEM)
    blocks = jax.ShapeDtypeStruct((count, slabs, 2, W, W), F32)
    out_spec = pl.BlockSpec((some, slabs, 2, W, W), lambda e: (e, 0, 0, 0, 0))
    packed, flow = pl.pallas_call(
        functools.partial(sure_kernel, fast),
        grid=(count // some,),
        out_shape=(blocks, jax.ShapeDtypeStruct((count // some, 8, W), F32)),
        in_specs=[
            pl.BlockSpec(memory_space=pltpu.SMEM),
            pl.BlockSpec((slabs, owners, 2, some, depth, W), lambda e: (0, 0, 0, e, 0, 0)),
            vmem,
            vmem,
        ],
        out_specs=(out_spec, pl.BlockSpec((1, 8, W), lambda e: (e, 0, 0))),
        scratch_shapes=Solver.scratch(some, slabs),
        compiler_params=pltpu.CompilerParams(vmem_limit_bytes=(44 if fast else 16) * 1024 * 1024),
        cost_estimate=pl.CostEstimate(flops=20_000_000_000, bytes_accessed=8_000_000, transcendentals=0),
    )(scalars, sigma, hamiltonian, coupling)
    return packed, jnp.sum(flow, axis=0)


def spread_kernel(packed_ref, less_ref, great_ref):
    rows = lax.broadcasted_iota(jnp.int32, (W, W), 0)
    cols = lax.broadcasted_iota(jnp.int32, (W, W), 1)
    for slab in range(packed_ref.shape[1]):
        for kind, ref in enumerate((less_ref, great_ref)):
            real, imag = unpacked(packed_ref[0, slab, kind], rows, cols)
            ref[0, slab, 0] = real
            ref[0, slab, 1] = imag


def spread(packed):
    spec = pl.BlockSpec((1,) + packed.shape[1:], lambda e: (e, 0, 0, 0, 0))
    return pl.pallas_call(
        spread_kernel,
        grid=(packed.shape[0],),
        out_shape=(jax.ShapeDtypeStruct(packed.shape, F32),) * 2,
        in_specs=[spec],
        out_specs=(spec, spec),
        compiler_params=pltpu.CompilerParams(vmem_limit_bytes=16 * 1024 * 1024),
    )(packed)


MESH = pl.DeviceIdType.MESH
GATHERED = 2


def remote(source, target, send_sem, recv_sem, peer):
    return pltpu.make_async_remote_copy(
        src_ref=source, dst_ref=target, send_sem=send_sem, recv_sem=recv_sem,
        device_id=peer, device_id_type=MESH,
    )


def exchange_kernel(
    by, n_energy, n_mom,
    weight_ref, less_hbm, great_hbm, sigma_ref,
    less_ref, great_ref, load_sem, pack, near_a, near_b, half_a, half_b, share, high, low, send_sem, recv_sem,
):
    place = lax.axis_index("energy")
    me = lax.axis_index("mom")
    slabs, count = less_ref.shape[:2]
    depth = W // n_mom
    loads = [
        [
            pltpu.make_async_copy(source.at[:, c], target.at[c], load_sem.at[kind, c])
            for kind, (source, target) in enumerate(((less_hbm, less_ref), (great_hbm, great_ref)))
        ]
        for c in range(slabs)
    ]
    for c in range(slabs - 1, -1, -1):
        for load in loads[c]:
            load.start()
    after = lax.rem(me + 1, n_mom)
    before = lax.rem(me + n_mom - 1, n_mom)
    across = lax.rem(me + 2, n_mom)
    over = {"energy": lax.rem(place + by, n_energy)}
    under = {"energy": lax.rem(place - by + n_energy, n_energy)}
    wrapped_up = lax.div(place + by, n_energy)
    wrapped_down = 1 - lax.div(place - by + n_energy, n_energy)
    kept_up = (1 - wrapped_up).astype(F32)
    kept_down = (1 - wrapped_down).astype(F32)
    emission = weight_ref[0] * (1.0 / n_mom)
    absorption = weight_ref[1] * (1.0 / n_mom)

    barrier = pltpu.get_barrier_semaphore()
    for peer in ({"mom": after}, {"mom": before}, over, under):
        pl.semaphore_signal(barrier, inc=1, device_id=peer, device_id_type=MESH)

    def send(kind, chunk, source, target, peer):
        copy = remote(source, target, send_sem.at[kind, chunk], recv_sem.at[kind, chunk], peer)
        copy.start()
        return copy

    sent = {}

    def pass_on(c):
        sent[6, c].wait_recv()
        part = sigma_ref.at[c, before, 0]
        sent[8, c] = send(8, c, part, part, {"mom": after})
        sent[7, c].wait_recv()
        part = sigma_ref.at[c, after, 1]
        sent[9, c] = send(9, c, part, part, {"mom": before})

    rows = lax.broadcasted_iota(jnp.int32, (depth, W), 0)
    cols = lax.broadcasted_iota(jnp.int32, (depth, W), 1)
    order = range(slabs - 1, -1, -1)
    for c in order:
        for load in loads[c]:
            load.wait()
        for part in range(n_mom):
            span = slice(part * depth, (part + 1) * depth)
            upper = cols > rows + part * depth
            for kind, ref in enumerate((less_ref, great_ref)):
                pack[c, part, kind] = jnp.where(upper, ref[c, :, 0, span], ref[c, :, 1, span])
        if c == slabs - 1:
            pl.semaphore_wait(barrier, 4)
        sent[0, c] = send(0, c, pack.at[c, across, 0], near_a.at[c], {"mom": after})
        sent[1, c] = send(1, c, pack.at[c, across, 1], near_b.at[c], {"mom": before})
    for c in order:
        sent[0, c].wait_recv()
        pack[c, after, 0] = pack[c, after, 0] + near_a[c]
        sent[1, c].wait_recv()
        pack[c, before, 1] = pack[c, before, 1] + near_b[c]
        sent[2, c] = send(2, c, pack.at[c, after], half_a.at[c], {"mom": after})
        sent[3, c] = send(3, c, pack.at[c, before], half_b.at[c], {"mom": before})
    for c in order:
        sent[2, c].wait_recv()
        sent[3, c].wait_recv()
        share[c] = pack[c, me] + (half_a[c] + half_b[c])
        sent[4, c] = send(4, c, share.at[c], high.at[c], under)
        sent[5, c] = send(5, c, share.at[c], low.at[c], over)
    for c in order:
        sent[4, c].wait_recv()
        sent[5, c].wait_recv()
        for j in range(count):
            if j < count - 1:
                up = [high[c, kind, j + wrapped_up] for kind in range(2)]
            else:
                up = [high[c, kind, j] * kept_up for kind in range(2)]
            if j > 0:
                down = [low[c, kind, j - wrapped_down] for kind in range(2)]
            else:
                down = [low[c, kind, j] * kept_down for kind in range(2)]
            sigma_ref[c, me, 0, j] = emission * up[0] + absorption * down[0]
            sigma_ref[c, me, 1, j] = emission * down[1] + absorption * up[1]
        if c >= slabs - GATHERED:
            mine = sigma_ref.at[c, me]
            sent[6, c] = send(6, c, mine, mine, {"mom": after})
            sent[7, c] = send(7, c, mine, mine, {"mom": before})
        if c + 1 < slabs and c + 1 >= slabs - GATHERED:
            pass_on(c + 1)
    for c in order:
        if (8, c) in sent:
            sent[8, c].wait_recv()
            sent[9, c].wait_recv()
    for copy in sent.values():
        copy.wait_send()


def exchange(by, n_energy, n_mom, weight, lesser, greater):
    count, slabs = lesser.shape[:2]
    depth = W // n_mom
    vmem = pl.BlockSpec(memory_space=pltpu.VMEM)
    hbm = pl.BlockSpec(memory_space=pl.ANY)
    block = pltpu.VMEM((slabs, count, 2, W, W), F32)
    half = pltpu.VMEM((slabs, count, depth, W), F32)
    whole = pltpu.VMEM((slabs, 2, count, depth, W), F32)
    return pl.pallas_call(
        functools.partial(exchange_kernel, by, n_energy, n_mom),
        out_shape=jax.ShapeDtypeStruct((slabs, n_mom, 2, count, depth, W), F32),
        in_specs=[pl.BlockSpec(memory_space=pltpu.SMEM), hbm, hbm],
        out_specs=vmem,
        scratch_shapes=[
            block, block, pltpu.SemaphoreType.DMA((2, slabs)),
            pltpu.VMEM((slabs, n_mom, 2, count, depth, W), F32),
            half, half, whole, whole, whole, whole, whole,
            pltpu.SemaphoreType.DMA((10, slabs)),
            pltpu.SemaphoreType.DMA((10, slabs)),
        ],
        compiler_params=pltpu.CompilerParams(
            collective_id=by, has_side_effects=True, vmem_limit_bytes=32 * 1024 * 1024
        ),
    )(weight, lesser, greater)


def fast_kernel(
    n_mom, inner, outer,
    scal_ref, share_ref, ham_ref, hop_ref, out_ref, flow_ref, missed_ref,
    sigma, first, second, tile, partial, send_sem, recv_sem, sum_send, sum_recv, *scratch,
):
    solver = Solver(True, rows_of(sigma), scal_ref, ham_ref, out_ref, scratch)
    slabs = solver.slabs
    place = lax.axis_index("energy")
    me = lax.axis_index("mom")
    after = lax.rem(me + 1, n_mom)
    before = lax.rem(me + n_mom - 1, n_mom)
    low = lax.rem(place, inner)
    high = lax.div(place, inner)
    slot = high * n_mom + me

    def outer_peer(step):
        other = lax.rem(slot + step, outer)
        return other, {"energy": lax.div(other, n_mom) * inner + low, "mom": lax.rem(other, n_mom)}

    def inner_peer(step):
        other = lax.rem(low + step, inner)
        return other, {"energy": high * inner + other, "mom": me}

    barrier = pltpu.get_barrier_semaphore()
    for step in range(1, outer):
        pl.semaphore_signal(barrier, inc=1, device_id=outer_peer(step)[1], device_id_type=MESH)
    for step in range(1, inner):
        pl.semaphore_signal(barrier, inc=1, device_id=inner_peer(step)[1], device_id_type=MESH)

    def near(slab):
        for kind, peer in ((0, after), (1, before)):
            yield remote(
                share_ref.at[slab, me], sigma.at[slab, me],
                send_sem.at[kind, slab], recv_sem.at[kind, slab], {"mom": peer},
            )

    def far(slab):
        for kind, owner, peer in ((0, before, after), (1, after, before)):
            part = sigma.at[slab, owner, kind]
            yield remote(
                part, part, send_sem.at[2 + kind, slab], recv_sem.at[2 + kind, slab], {"mom": peer}
            )

    def started(copies):
        for copy in copies:
            copy.start()

    def arrived(copies):
        for copy in copies:
            copy.wait_recv()

    rest = range(slabs - GATHERED - 1, -1, -1)

    def share_rest():
        pl.semaphore_wait(barrier, outer + inner - 2)
        for slab in range(slabs - GATHERED, slabs - 1):
            sigma[slab] = share_ref[slab]
        for slab in rest:
            started(near(slab))
            sigma[slab, me] = share_ref[slab, me]

    solver.start(hop_ref)
    solver.level(slabs - 1, True, share_rest, rows_of(share_ref))

    def down(step, carry):
        slab = slabs - 2 - step

        def pass_on():
            @pl.when(step == 0)
            def _():
                for other in rest:
                    arrived(near(other))
                    started(far(other))

        solver.fold(slab + 1)

        @pl.when(slab < slabs - GATHERED)
        def _():
            arrived(far(slab))

        solver.level(slab, False, pass_on)
        return carry

    lax.fori_loop(0, slabs - 1, down, 0)

    def round_of(source, slots, size, own, peer, base):
        def copy(index, step):
            return remote(
                source, slots.at[index], sum_send.at[base + step], sum_recv.at[base + index], peer(step)[1]
            )

        def begin():
            for step in range(1, size):
                copy(own, step).start()
            slots[own] = source[...]

        def end():
            for step in range(1, size):
                copy(peer(step)[0], step).wait_recv()
            result = slots[0]
            for index in range(1, size):
                result = result + slots[index]
            for step in range(1, size):
                copy(own, step).wait_send()
            return result

        return begin, end

    begin_outer, end_outer = round_of(tile, first, outer, slot, outer_peer, 0)
    begin_inner, end_inner = round_of(partial, second, inner, low, inner_peer, outer)
    tile[...] = solver.flow()
    solver.first()
    begin_outer()
    for slab in range(1, slabs - 1):
        solver.up(slab)
    partial[...] = end_outer()
    begin_inner()
    solver.up(slabs - 1)
    total = end_inner()
    flow_ref[...] = total[0:1, 0:1]
    missed_ref[...] = jnp.where(total[1:2, 0:1] > 0.5, 1, 0)
    for slab in rest:
        for copies in (near(slab), far(slab)):
            for copy in copies:
                copy.wait_send()


def quick(n_energy, n_mom, scalars, share, hamiltonian, coupling, inner=8):
    slabs, _, _, count, depth = share.shape[:5]
    outer = n_energy // inner * n_mom
    vmem = pl.BlockSpec(memory_space=pltpu.VMEM)
    blocks = jax.ShapeDtypeStruct((count, slabs, 2, W, W), F32)
    return pl.pallas_call(
        functools.partial(fast_kernel, n_mom, inner, outer),
        out_shape=(
            blocks,
            jax.ShapeDtypeStruct((1, 1), F32),
            jax.ShapeDtypeStruct((1, 1), jnp.int32),
        ),
        in_specs=[pl.BlockSpec(memory_space=pltpu.SMEM), vmem, vmem, vmem],
        out_specs=(vmem, vmem, vmem),
        scratch_shapes=[
            pltpu.VMEM((slabs, n_mom, 2, count, depth, W), F32),
            pltpu.VMEM((outer, 8, W), F32),
            pltpu.VMEM((inner, 8, W), F32),
            pltpu.VMEM((8, W), F32),
            pltpu.VMEM((8, W), F32),
            pltpu.SemaphoreType.DMA((4, slabs)),
            pltpu.SemaphoreType.DMA((4, slabs)),
            pltpu.SemaphoreType.DMA((outer + inner,)),
            pltpu.SemaphoreType.DMA((outer + inner,)),
        ]
        + Solver.scratch(count, slabs),
        compiler_params=pltpu.CompilerParams(
            collective_id=SMAX + 1, has_side_effects=True, vmem_limit_bytes=26 * 1024 * 1024
        ),
    )(scalars, share, hamiltonian, coupling)


def moved(array, axis, by):
    size = lax.axis_size(axis)
    return lax.ppermute(array, axis, [(i, (i + by) % size) for i in range(size)]) if by else array


def shards(lesser, greater, hamiltonian, coupling, shift, phonon_weight):
    n_energy = lax.axis_size("energy")
    n_mom = lax.axis_size("mom")
    here = lax.axis_index("energy")
    count = lesser.shape[0]
    total = count * n_energy
    branches = [functools.partial(exchange, k + 1, n_energy, n_mom) for k in range(SMAX)]
    share = lax.switch(shift[0] - 1, branches, phonon_weight, lesser[:, 0, 0], greater[:, 0, 0])
    grid = (jnp.arange(count) * n_energy + here).astype(F32)
    energy = (grid + 0.5) * (2.0 * band_edge / total) - band_edge
    scalars = jnp.stack(
        [
            energy,
            jax.nn.sigmoid((left_level - energy) / thermal),
            jax.nn.sigmoid((right_level - energy) / thermal),
        ]
    )
    ham, hop = hamiltonian[0], coupling[0]
    packed, flow, missed = quick(n_energy, n_mom, scalars, share, ham, hop)

    def again(share, packed, flow):
        mine = share[:, lax.axis_index("mom")]
        parts = jnp.stack([moved(mine, "mom", k) for k in range(n_mom)], 1)
        owners = (lax.axis_index("mom") - jnp.arange(n_mom)) % n_mom
        sigma = jnp.zeros_like(parts).at[:, owners].set(parts)
        packed, tile = transport(scalars, sigma, ham, hop)
        flow = tile[0, 0]
        for axis, size in (("mom", n_mom), ("energy", n_energy)):
            by = 1
            while by < size:
                flow = flow + lax.ppermute(flow, axis, [(i, i ^ by) for i in range(size)])
                by = 2 * by
        return (*spread(packed), flow)

    def keep(share, packed, flow):
        return (*spread(packed), flow.reshape(()))

    branch = missed.reshape(())
    less_new, great_new, current = lax.switch(branch, [keep, again], share, packed, flow)
    return (less_new[:, None, None], great_new[:, None, None], current)


def solution(mesh):
    return jax.shard_map(
        shards,
        mesh=mesh,
        in_specs=(
            P(None, "energy", "mom", None, None, None, None),
            P(None, "energy", "mom", None, None, None, None),
            P("mom", None, None, None, None),
            P("mom", None, None, None),
            P(),
            P(),
        ),
        out_specs=(
            P(None, "energy", "mom", None, None, None, None),
            P(None, "energy", "mom", None, None, None, None),
            P(),
        ),
        check_vma=False,
    )
```

```python
import functools

import jax
import jax.numpy as jnp
from jax import lax
from jax.experimental import pallas as pl
from jax.experimental.pallas import tpu as pltpu
from jax.sharding import PartitionSpec as P

SMAX = 7
POINTS = 128
broaden = 0.2
contact_rate = 0.5
left_level = 0.3
right_level = -0.3
thermal = 0.1
band_edge = 2.0

W = 128
BF = jnp.bfloat16
F32 = jnp.float32
LEAST = 0.03


def store(ref, real, imag):
    for row, part in ((0, real), (W, imag)):
        high = part.astype(BF)
        ref[row : row + W, :W] = high
        ref[row : row + W, W:] = (part - high.astype(F32)).astype(BF)


def store_high(ref, real, imag):
    ref[:W, :W] = real.astype(BF)
    ref[W:, :W] = imag.astype(BF)


def unpacked(value, rows, cols):
    turned = value.T
    real = jnp.where(rows < cols, value, jnp.where(rows > cols, -turned, 0.0))
    imag = jnp.where(rows >= cols, value, turned)
    return real, imag


def twofold(ref, column):
    real, imag = ref[:W, column : column + W], ref[W:, column : column + W]
    return jnp.concatenate([jnp.concatenate([real, imag], 1), jnp.concatenate([-imag, real], 1)], 0)


def product(left, right, dagger=False, high=False):
    dims = (((1,), (1,)), ((), ())) if dagger else (((1,), (0,)), ((), ()))
    top = jnp.concatenate([left[:W, :W], left[W:, :W]], 1)
    if high:
        full = lax.dot_general(top, twofold(right, 0), dims, preferred_element_type=F32)
        return full[:, :W], full[:, W:]
    bottom = jnp.concatenate([left[:W, W:], left[W:, W:]], 1)
    both = jnp.concatenate([top, bottom], 0)
    full = lax.dot_general(both, twofold(right, 0), dims, preferred_element_type=F32)
    rest = lax.dot_general(top, twofold(right, W), dims, preferred_element_type=F32)
    full = full[:W] + full[W:] + rest
    return full[:, :W], full[:, W:]


FAST_LOW = 0.006
FAST_TOP = 0.4
FAST_GROW = 5
FAST_REFINE = 2
RESIDUAL = 1.0e-4


def schedule():
    lowest, steps = FAST_LOW, []
    for step in range(FAST_GROW):
        used = max(lowest, LEAST)
        a = 4.0 / (1.0 + used)
        b = a / (1.0 + used)
        lowest = min(lowest * (a - b * lowest), b * used)
        centre = 2.0 / (1.0 + lowest) if step == FAST_GROW - 1 else 1.0
        steps.append((a * centre, b * centre))
    return steps


class Solver:
    names = (
        "hop_f", "sys_f", "inv_f", "tmp_f", "inj_f", "gr_f", "t_f", "l_f", "full_f",
        "inv", "gl", "gr", "rho",
    )

    def __init__(self, fast, sigma, scal, ham, out, scratch, base=0):
        self.fast = fast
        self.sigma = sigma
        self.scal = lambda row, e: scal[row, base + e]
        self.ham = ham
        self.out = out
        for name, ref in zip(self.names, scratch, strict=True):
            setattr(self, name, ref)
        self.count = self.inv.shape[0]
        self.weight = 2.0 * band_edge / POINTS
        self.slabs = ham.shape[0]
        self.energies = range(self.count)
        self.rows = lax.broadcasted_iota(jnp.int32, (W, W), 0)
        self.cols = lax.broadcasted_iota(jnp.int32, (W, W), 1)
        self.eye = jnp.where(self.rows == self.cols, 1.0, 0.0).astype(F32)

    @classmethod
    def scratch(cls, count, slabs):
        form = (2 * W, 2 * W)
        blocks = (count, 2, W, W)
        few = pltpu.VMEM((count,) + form, BF)
        many = pltpu.VMEM((slabs, count) + form, BF)
        every = pltpu.VMEM((slabs,) + blocks, F32)
        own = pltpu.VMEM(blocks, F32)
        return [
            pltpu.VMEM(form, BF), few, few, few, few, many, many, many,
            pltpu.VMEM((2, count) + form, BF), own, every, every, pltpu.VMEM((8, W), F32),
        ]

    def start(self, hop):
        store(self.hop_f, hop[0].T, -hop[1].T)
        self.rho[...] = jnp.zeros((8, W), F32)

    def block(self, sigma, slab, kind, e):
        return unpacked(sigma(slab, kind, e), self.rows, self.cols)

    def grow_step(self, a, b):
        for e in self.energies:
            real, imag = product(self.inv_f.at[e], self.sys_f.at[e], high=True)
            store_high(self.tmp_f.at[e], real, imag)
        for e in self.energies:
            real, imag = product(self.tmp_f.at[e], self.inv_f.at[e], high=True)
            real = a * self.inv[e, 0] - b * real
            imag = a * self.inv[e, 1] - b * imag
            self.inv[e, 0] = real
            self.inv[e, 1] = imag
            store_high(self.inv_f.at[e], real, imag)

    def whole_form(self):
        for e in self.energies:
            store(self.inv_f.at[e], self.inv[e, 0], self.inv[e, 1])

    def refine_step(self, slab=None):
        sizes = []
        for e in self.energies:
            real, imag = product(self.inv_f.at[e], self.sys_f.at[e])
            real = self.eye - real
            sizes.append(jnp.sum(real * real + imag * imag, axis=0, keepdims=True))
            store_high(self.tmp_f.at[e], real, -imag)
        for e in self.energies:
            real, imag = product(self.tmp_f.at[e], self.inv_f.at[e], high=True)
            real = self.inv[e, 0] + real
            imag = self.inv[e, 1] + imag
            place = (e,) if slab is None else (slab, e)
            values, form = (self.inv, self.inv_f) if slab is None else (self.gr, self.gr_f)
            values[(*place, 0)] = real
            values[(*place, 1)] = imag
            store(form.at[place], real, imag)
        return sizes

    def invert(self, slab, midway):
        norms = []
        for e in self.energies:
            real, imag = product(self.inv_f.at[e], self.sys_f.at[e], high=True)
            norms.append(jnp.sum(jnp.sqrt(real * real + imag * imag), axis=0, keepdims=True))
            if self.fast:
                store_high(self.tmp_f.at[e], real, imag)
        bound = 1.05 * jnp.max(functools.reduce(jnp.maximum, norms))
        if self.fast:
            steps = schedule()
            scale = 1.0 / (FAST_TOP * bound)
            first = steps[0][0] * scale
            second = steps[0][1] * scale * scale
            for e in self.energies:
                real, imag = product(self.tmp_f.at[e], self.inv_f.at[e], high=True)
                real = first * self.inv[e, 0] - second * real
                imag = first * self.inv[e, 1] - second * imag
                self.inv[e, 0] = real
                self.inv[e, 1] = imag
                store_high(self.inv_f.at[e], real, imag)
            for place, (a, b) in enumerate(steps[1:]):
                self.grow_step(a, b)
                if place == 1 and midway is not None:
                    midway()
            self.whole_form()
            for step in range(FAST_REFINE):
                sizes = self.refine_step(slab if step == FAST_REFINE - 1 else None)
            self.rho[0:1] = self.rho[0:1] + functools.reduce(jnp.add, sizes)
            return
        scale = 1.0 / bound
        for e in self.energies:
            real = self.inv[e, 0] * scale
            imag = self.inv[e, 1] * scale
            self.inv[e, 0] = real
            self.inv[e, 1] = imag
        self.whole_form()

        def grow(carry):
            lowest, done = carry
            used = jnp.maximum(lowest, LEAST)
            a = 4.0 / (1.0 + used)
            b = a / (1.0 + used)
            after = jnp.minimum(lowest * (a - b * lowest), b * used)
            for e in self.energies:
                real, imag = product(self.inv_f.at[e], self.sys_f.at[e])
                store(self.tmp_f.at[e], real, imag)
            for e in self.energies:
                real, imag = product(self.tmp_f.at[e], self.inv_f.at[e])
                real = a * self.inv[e, 0] - b * real
                imag = a * self.inv[e, 1] - b * imag
                self.inv[e, 0] = real
                self.inv[e, 1] = imag
                store(self.inv_f.at[e], real, imag)
            return after, done + 1

        lax.while_loop(
            lambda carry: jnp.logical_and(carry[0] < 0.9, carry[1] < 64),
            grow,
            (broaden * broaden * scale, jnp.int32(0)),
        )

        def refine(carry):
            sizes = [jnp.sum(size) for size in self.refine_step()]
            return functools.reduce(jnp.maximum, sizes), carry[1] + 1

        lax.while_loop(
            lambda carry: jnp.logical_and(carry[0] > 4.0e-6, carry[1] < 24),
            refine,
            (jnp.float32(1.0), jnp.int32(0)),
        )

    def level(self, slab, last, midway=None, sigma=None):
        sigma = self.sigma if sigma is None else sigma
        at_left = 0.0 if last else jnp.where(slab == 0, 1.0, 0.0)
        for e in self.energies:
            less = self.block(sigma, slab, 0, e)
            great = self.block(sigma, slab, 1, e)
            fill = self.scal(2, e) if last else at_left * self.scal(1, e)
            contact = contact_rate if last else at_left * contact_rate
            sys_r = self.scal(0, e) * self.eye - self.ham[slab, 0] - 0.5 * (great[0] - less[0])
            sys_i = (broaden + contact) * self.eye - self.ham[slab, 1] - 0.5 * (great[1] - less[1])
            inj_r = less[0]
            inj_i = less[1] + 2.0 * contact_rate * fill * self.eye
            if not last:
                real, imag = product(self.t_f.at[slab + 1, e], self.hop_f, dagger=True)
                sys_r = sys_r - real
                sys_i = sys_i - imag
                real, imag = product(self.l_f.at[slab + 1, e], self.hop_f, dagger=True)
                inj_r = inj_r + real
                inj_i = inj_i + imag
            store(self.sys_f.at[e], sys_r, sys_i)
            store(self.inj_f.at[e], inj_r, inj_i)
            back_r = sys_r.T
            back_i = -sys_i.T
            self.inv[e, 0] = back_r
            self.inv[e, 1] = back_i
            store_high(self.inv_f.at[e], back_r, back_i)
        self.invert(slab, midway)
        for e in self.energies:
            if not self.fast:
                self.gr[slab, e] = self.inv[e]
                self.gr_f[slab, e] = self.inv_f[e]
            real, imag = product(self.gr_f.at[slab, e], self.inj_f.at[e])
            store(self.tmp_f.at[e], real, imag)
        for e in self.energies:
            real, imag = product(self.tmp_f.at[e], self.gr_f.at[slab, e], dagger=True)
            self.gl[slab, e, 0] = real
            self.gl[slab, e, 1] = imag
            store(self.inj_f.at[e], real, imag)

    def fold(self, slab):
        for e in self.energies:
            real, imag = product(self.hop_f, self.gr_f.at[slab, e])
            store(self.t_f.at[slab, e], real, imag)
            real, imag = product(self.hop_f, self.inj_f.at[e])
            store(self.l_f.at[slab, e], real, imag)

    def flow(self):
        flow = jnp.zeros((1, W), F32)
        for e in self.energies:
            fill = self.scal(1, e)
            less = self.gl[0, e, 1]
            mixed = fill * (less + 2.0 * self.gr[0, e, 1]) + (1.0 - fill) * less
            flow = flow - jnp.sum(mixed * self.eye, axis=0, keepdims=True)
        flow = jnp.broadcast_to(jnp.sum(flow, axis=1, keepdims=True) * self.weight, (8, W))
        missed = jnp.broadcast_to(jnp.sum(self.rho[0:1], axis=1, keepdims=True), (8, W))
        missed = jnp.where(missed <= RESIDUAL, 0.0, 1.0)
        return jnp.where(lax.broadcasted_iota(jnp.int32, (8, W), 0) == 0, flow, missed)

    def finish(self, slab, e, green, less):
        great = (less[0] + green[0] - green[0].T, less[1] + green[1] + green[1].T)
        upper = self.rows < self.cols
        self.out[e, slab, 0] = jnp.where(upper, less[0], less[1])
        self.out[e, slab, 1] = jnp.where(upper, great[0], great[1])
        store(self.full_f.at[0, e], *green)
        store(self.full_f.at[1, e], *less)

    def first(self):
        for e in self.energies:
            self.finish(0, e, (self.gr[0, e, 0], self.gr[0, e, 1]), (self.gl[0, e, 0], self.gl[0, e, 1]))

    def up(self, slab):
        for e in self.energies:
            real, imag = product(self.gr_f.at[slab, e], self.hop_f, dagger=True)
            store(self.sys_f.at[e], real, imag)
        for e in self.energies:
            real, imag = product(self.sys_f.at[e], self.full_f.at[0, e])
            store(self.tmp_f.at[e], real, imag)
            real, imag = product(self.sys_f.at[e], self.full_f.at[1, e])
            store(self.inj_f.at[e], real, imag)
        for e in self.energies:
            real, imag = product(self.tmp_f.at[e], self.t_f.at[slab, e])
            green = (self.gr[slab, e, 0] + real, self.gr[slab, e, 1] + imag)
            cross = product(self.tmp_f.at[e], self.l_f.at[slab, e])
            real, imag = product(self.inj_f.at[e], self.sys_f.at[e], dagger=True)
            less = (
                self.gl[slab, e, 0] + real + cross[0] - cross[0].T,
                self.gl[slab, e, 1] + imag + cross[1] + cross[1].T,
            )
            self.finish(slab, e, green, less)


def rows_of(sigma_ref):
    def read(slab, kind, e):
        return jnp.concatenate([sigma_ref[slab, owner, kind, e] for owner in range(sigma_ref.shape[1])], 0)

    return read


def sure_kernel(fast, scal_ref, sig_ref, ham_ref, hop_ref, out_ref, flow_ref, *scratch):
    base = pl.program_id(0) * sig_ref.shape[3]
    solver = Solver(fast, rows_of(sig_ref), scal_ref, ham_ref, out_ref, scratch, base)
    slabs = solver.slabs
    solver.start(hop_ref)
    solver.level(slabs - 1, True)

    def down(step, carry):
        slab = slabs - 2 - step
        solver.fold(slab + 1)
        solver.level(slab, False)
        return carry

    lax.fori_loop(0, slabs - 1, down, 0)
    flow_ref[0] = solver.flow()
    solver.first()

    def up(slab, carry):
        solver.up(slab)
        return carry

    lax.fori_loop(1, slabs, up, 0)


def transport(scalars, sigma, hamiltonian, coupling, fast=False):
    slabs, owners, _, count, depth = sigma.shape[:5]
    some = count if fast else 1
    vmem = pl.BlockSpec(memory_space=pltpu.VMEM)
    blocks = jax.ShapeDtypeStruct((count, slabs, 2, W, W), F32)
    out_spec = pl.BlockSpec((some, slabs, 2, W, W), lambda e: (e, 0, 0, 0, 0))
    packed, flow = pl.pallas_call(
        functools.partial(sure_kernel, fast),
        grid=(count // some,),
        out_shape=(blocks, jax.ShapeDtypeStruct((count // some, 8, W), F32)),
        in_specs=[
            pl.BlockSpec(memory_space=pltpu.SMEM),
            pl.BlockSpec((slabs, owners, 2, some, depth, W), lambda e: (0, 0, 0, e, 0, 0)),
            vmem,
            vmem,
        ],
        out_specs=(out_spec, pl.BlockSpec((1, 8, W), lambda e: (e, 0, 0))),
        scratch_shapes=Solver.scratch(some, slabs),
        compiler_params=pltpu.CompilerParams(vmem_limit_bytes=(44 if fast else 16) * 1024 * 1024),
        cost_estimate=pl.CostEstimate(flops=20_000_000_000, bytes_accessed=8_000_000, transcendentals=0),
    )(scalars, sigma, hamiltonian, coupling)
    return packed, jnp.sum(flow, axis=0)


def spread_kernel(packed_ref, less_ref, great_ref):
    rows = lax.broadcasted_iota(jnp.int32, (W, W), 0)
    cols = lax.broadcasted_iota(jnp.int32, (W, W), 1)
    for slab in range(packed_ref.shape[1]):
        for kind, ref in enumerate((less_ref, great_ref)):
            real, imag = unpacked(packed_ref[0, slab, kind], rows, cols)
            ref[0, slab, 0] = real
            ref[0, slab, 1] = imag


def spread(packed):
    spec = pl.BlockSpec((1,) + packed.shape[1:], lambda e: (e, 0, 0, 0, 0))
    return pl.pallas_call(
        spread_kernel,
        grid=(packed.shape[0],),
        out_shape=(jax.ShapeDtypeStruct(packed.shape, F32),) * 2,
        in_specs=[spec],
        out_specs=(spec, spec),
        compiler_params=pltpu.CompilerParams(vmem_limit_bytes=16 * 1024 * 1024),
    )(packed)


MESH = pl.DeviceIdType.MESH
GATHERED = 2


def remote(source, target, send_sem, recv_sem, peer):
    return pltpu.make_async_remote_copy(
        src_ref=source, dst_ref=target, send_sem=send_sem, recv_sem=recv_sem,
        device_id=peer, device_id_type=MESH,
    )


def exchange_kernel(
    by, n_energy, n_mom,
    weight_ref, less_hbm, great_hbm, sigma_ref,
    less_ref, great_ref, load_sem, pack, near_a, near_b, half_a, half_b, share, high, low, send_sem, recv_sem,
):
    place = lax.axis_index("energy")
    me = lax.axis_index("mom")
    slabs, count = less_ref.shape[:2]
    depth = W // n_mom
    loads = [
        [
            pltpu.make_async_copy(source.at[:, c], target.at[c], load_sem.at[kind, c])
            for kind, (source, target) in enumerate(((less_hbm, less_ref), (great_hbm, great_ref)))
        ]
        for c in range(slabs)
    ]
    for c in range(slabs - 1, -1, -1):
        for load in loads[c]:
            load.start()
    after = lax.rem(me + 1, n_mom)
    before = lax.rem(me + n_mom - 1, n_mom)
    across = lax.rem(me + 2, n_mom)
    over = {"energy": lax.rem(place + by, n_energy)}
    under = {"energy": lax.rem(place - by + n_energy, n_energy)}
    wrapped_up = lax.div(place + by, n_energy)
    wrapped_down = 1 - lax.div(place - by + n_energy, n_energy)
    kept_up = (1 - wrapped_up).astype(F32)
    kept_down = (1 - wrapped_down).astype(F32)
    emission = weight_ref[0] * (1.0 / n_mom)
    absorption = weight_ref[1] * (1.0 / n_mom)

    barrier = pltpu.get_barrier_semaphore()
    for peer in ({"mom": after}, {"mom": before}, over, under):
        pl.semaphore_signal(barrier, inc=1, device_id=peer, device_id_type=MESH)

    def send(kind, chunk, source, target, peer):
        copy = remote(source, target, send_sem.at[kind, chunk], recv_sem.at[kind, chunk], peer)
        copy.start()
        return copy

    sent = {}

    def pass_on(c):
        sent[6, c].wait_recv()
        part = sigma_ref.at[c, before, 0]
        sent[8, c] = send(8, c, part, part, {"mom": after})
        sent[7, c].wait_recv()
        part = sigma_ref.at[c, after, 1]
        sent[9, c] = send(9, c, part, part, {"mom": before})

    rows = lax.broadcasted_iota(jnp.int32, (depth, W), 0)
    cols = lax.broadcasted_iota(jnp.int32, (depth, W), 1)
    order = range(slabs - 1, -1, -1)
    for c in order:
        for load in loads[c]:
            load.wait()
        for part in range(n_mom):
            span = slice(part * depth, (part + 1) * depth)
            upper = cols > rows + part * depth
            for kind, ref in enumerate((less_ref, great_ref)):
                pack[c, part, kind] = jnp.where(upper, ref[c, :, 0, span], ref[c, :, 1, span])
        if c == slabs - 1:
            pl.semaphore_wait(barrier, 4)
        sent[0, c] = send(0, c, pack.at[c, across, 0], near_a.at[c], {"mom": after})
        sent[1, c] = send(1, c, pack.at[c, across, 1], near_b.at[c], {"mom": before})
    for c in order:
        sent[0, c].wait_recv()
        pack[c, after, 0] = pack[c, after, 0] + near_a[c]
        sent[1, c].wait_recv()
        pack[c, before, 1] = pack[c, before, 1] + near_b[c]
        sent[2, c] = send(2, c, pack.at[c, after], half_a.at[c], {"mom": after})
        sent[3, c] = send(3, c, pack.at[c, before], half_b.at[c], {"mom": before})
    def settle(c):
        sent[2, c].wait_recv()
        sent[3, c].wait_recv()
        share[c] = pack[c, me] + (half_a[c] + half_b[c])
        sent[4, c] = send(4, c, share.at[c], high.at[c], under)
        sent[5, c] = send(5, c, share.at[c], low.at[c], over)
    def combine(c):
        sent[4, c].wait_recv()
        sent[5, c].wait_recv()
        for j in range(count):
            if j < count - 1:
                up = [high[c, kind, j + wrapped_up] for kind in range(2)]
            else:
                up = [high[c, kind, j] * kept_up for kind in range(2)]
            if j > 0:
                down = [low[c, kind, j - wrapped_down] for kind in range(2)]
            else:
                down = [low[c, kind, j] * kept_down for kind in range(2)]
            sigma_ref[c, me, 0, j] = emission * up[0] + absorption * down[0]
            sigma_ref[c, me, 1, j] = emission * down[1] + absorption * up[1]
        if c >= slabs - GATHERED:
            mine = sigma_ref.at[c, me]
            sent[6, c] = send(6, c, mine, mine, {"mom": after})
            sent[7, c] = send(7, c, mine, mine, {"mom": before})

    last = slabs - 1
    settle(last)
    for c in range(last - 1, -1, -1):
        settle(c)
        combine(c + 1)
    pass_on(last)
    combine(0)
    for kind, c in ((8, last), (9, last), *((kind, c) for c in range(slabs - GATHERED, last) for kind in (6, 7))):
        sent[kind, c].wait_recv()
    for copy in sent.values():
        copy.wait_send()


def exchange(by, n_energy, n_mom, weight, lesser, greater):
    count, slabs = lesser.shape[:2]
    depth = W // n_mom
    vmem = pl.BlockSpec(memory_space=pltpu.VMEM)
    hbm = pl.BlockSpec(memory_space=pl.ANY)
    block = pltpu.VMEM((slabs, count, 2, W, W), F32)
    half = pltpu.VMEM((slabs, count, depth, W), F32)
    whole = pltpu.VMEM((slabs, 2, count, depth, W), F32)
    return pl.pallas_call(
        functools.partial(exchange_kernel, by, n_energy, n_mom),
        out_shape=jax.ShapeDtypeStruct((slabs, n_mom, 2, count, depth, W), F32),
        in_specs=[pl.BlockSpec(memory_space=pltpu.SMEM), hbm, hbm],
        out_specs=vmem,
        scratch_shapes=[
            block, block, pltpu.SemaphoreType.DMA((2, slabs)),
            pltpu.VMEM((slabs, n_mom, 2, count, depth, W), F32),
            half, half, whole, whole, whole, whole, whole,
            pltpu.SemaphoreType.DMA((10, slabs)),
            pltpu.SemaphoreType.DMA((10, slabs)),
        ],
        compiler_params=pltpu.CompilerParams(
            collective_id=by, has_side_effects=True, vmem_limit_bytes=32 * 1024 * 1024
        ),
    )(weight, lesser, greater)


def fast_kernel(
    n_mom, inner, outer,
    scal_ref, share_ref, ham_ref, hop_ref, out_ref, flow_ref, missed_ref,
    sigma, first, second, tile, partial, send_sem, recv_sem, sum_send, sum_recv, *scratch,
):
    solver = Solver(True, rows_of(sigma), scal_ref, ham_ref, out_ref, scratch)
    slabs = solver.slabs
    place = lax.axis_index("energy")
    me = lax.axis_index("mom")
    after = lax.rem(me + 1, n_mom)
    before = lax.rem(me + n_mom - 1, n_mom)
    low = lax.rem(place, inner)
    high = lax.div(place, inner)
    slot = high * n_mom + me

    def outer_peer(step):
        other = lax.rem(slot + step, outer)
        return other, {"energy": lax.div(other, n_mom) * inner + low, "mom": lax.rem(other, n_mom)}

    def inner_peer(step):
        other = lax.rem(low + step, inner)
        return other, {"energy": high * inner + other, "mom": me}

    barrier = pltpu.get_barrier_semaphore()
    for step in range(1, outer):
        pl.semaphore_signal(barrier, inc=1, device_id=outer_peer(step)[1], device_id_type=MESH)
    for step in range(1, inner):
        pl.semaphore_signal(barrier, inc=1, device_id=inner_peer(step)[1], device_id_type=MESH)

    def near(slab):
        for kind, peer in ((0, after), (1, before)):
            yield remote(
                share_ref.at[slab, me], sigma.at[slab, me],
                send_sem.at[kind, slab], recv_sem.at[kind, slab], {"mom": peer},
            )

    def far(slab, source=sigma):
        for kind, owner, peer in ((0, before, after), (1, after, before)):
            yield remote(
                source.at[slab, owner, kind], sigma.at[slab, owner, kind], send_sem.at[2 + kind, slab], recv_sem.at[2 + kind, slab], {"mom": peer}
            )

    def started(copies):
        for copy in copies:
            copy.start()

    def arrived(copies):
        for copy in copies:
            copy.wait_recv()

    rest = range(slabs - GATHERED - 1, -1, -1)
    nearly = range(slabs - GATHERED, slabs - 1)

    def share_rest():
        pl.semaphore_wait(barrier, outer + inner - 2)
        for slab in nearly:
            started(far(slab, share_ref))
            for owner in (me, before, after):
                sigma[slab, owner] = share_ref[slab, owner]
        for slab in rest:
            started(near(slab))
            sigma[slab, me] = share_ref[slab, me]

    solver.start(hop_ref)
    solver.level(slabs - 1, True, share_rest, rows_of(share_ref))

    def down(step, carry):
        slab = slabs - 2 - step

        def pass_on(others):
            @pl.when(step == 0)
            def _():
                for other in others:
                    arrived(near(other))
                    started(far(other))

        solver.fold(slab + 1)
        pass_on(rest[:1])
        arrived(far(slab))
        solver.level(slab, False, lambda: pass_on(rest[1:]))
        return carry

    lax.fori_loop(0, slabs - 1, down, 0)

    def round_of(source, slots, size, own, peer, base):
        def copy(index, step):
            return remote(
                source, slots.at[index], sum_send.at[base + step], sum_recv.at[base + index], peer(step)[1]
            )

        def begin():
            for step in range(1, size):
                copy(own, step).start()
            slots[own] = source[...]

        def end():
            for step in range(1, size):
                copy(peer(step)[0], step).wait_recv()
            result = slots[0]
            for index in range(1, size):
                result = result + slots[index]
            for step in range(1, size):
                copy(own, step).wait_send()
            return result

        return begin, end

    begin_outer, end_outer = round_of(tile, first, outer, slot, outer_peer, 0)
    begin_inner, end_inner = round_of(partial, second, inner, low, inner_peer, outer)
    tile[...] = solver.flow()
    solver.first()
    begin_outer()
    for slab in range(1, slabs - 1):
        solver.up(slab)
    partial[...] = end_outer()
    begin_inner()
    solver.up(slabs - 1)
    total = end_inner()
    flow_ref[...] = total[0:1, 0:1]
    missed_ref[...] = jnp.where(total[1:2, 0:1] > 0.5, 1, 0)
    for slab in rest:
        for copy in near(slab):
            copy.wait_send()
    for slab in (*nearly, *rest):
        for copy in far(slab):
            copy.wait_send()


def quick(n_energy, n_mom, scalars, share, hamiltonian, coupling, inner=8):
    slabs, _, _, count, depth = share.shape[:5]
    outer = n_energy // inner * n_mom
    vmem = pl.BlockSpec(memory_space=pltpu.VMEM)
    blocks = jax.ShapeDtypeStruct((count, slabs, 2, W, W), F32)
    return pl.pallas_call(
        functools.partial(fast_kernel, n_mom, inner, outer),
        out_shape=(
            blocks,
            jax.ShapeDtypeStruct((1, 1), F32),
            jax.ShapeDtypeStruct((1, 1), jnp.int32),
        ),
        in_specs=[pl.BlockSpec(memory_space=pltpu.SMEM), vmem, vmem, vmem],
        out_specs=(vmem, vmem, vmem),
        scratch_shapes=[
            pltpu.VMEM((slabs, n_mom, 2, count, depth, W), F32),
            pltpu.VMEM((outer, 8, W), F32),
            pltpu.VMEM((inner, 8, W), F32),
            pltpu.VMEM((8, W), F32),
            pltpu.VMEM((8, W), F32),
            pltpu.SemaphoreType.DMA((4, slabs)),
            pltpu.SemaphoreType.DMA((4, slabs)),
            pltpu.SemaphoreType.DMA((outer + inner,)),
            pltpu.SemaphoreType.DMA((outer + inner,)),
        ]
        + Solver.scratch(count, slabs),
        compiler_params=pltpu.CompilerParams(
            collective_id=SMAX + 1, has_side_effects=True, vmem_limit_bytes=26 * 1024 * 1024
        ),
    )(scalars, share, hamiltonian, coupling)


def moved(array, axis, by):
    size = lax.axis_size(axis)
    return lax.ppermute(array, axis, [(i, (i + by) % size) for i in range(size)]) if by else array


def shards(lesser, greater, hamiltonian, coupling, shift, phonon_weight):
    n_energy = lax.axis_size("energy")
    n_mom = lax.axis_size("mom")
    here = lax.axis_index("energy")
    count = lesser.shape[0]
    total = count * n_energy
    branches = [functools.partial(exchange, k + 1, n_energy, n_mom) for k in range(SMAX)]
    share = lax.switch(shift[0] - 1, branches, phonon_weight, lesser[:, 0, 0], greater[:, 0, 0])
    grid = (jnp.arange(count) * n_energy + here).astype(F32)
    energy = (grid + 0.5) * (2.0 * band_edge / total) - band_edge
    scalars = jnp.stack(
        [
            energy,
            jax.nn.sigmoid((left_level - energy) / thermal),
            jax.nn.sigmoid((right_level - energy) / thermal),
        ]
    )
    ham, hop = hamiltonian[0], coupling[0]
    packed, flow, missed = quick(n_energy, n_mom, scalars, share, ham, hop)

    def again(share, packed, flow):
        mine = share[:, lax.axis_index("mom")]
        parts = jnp.stack([moved(mine, "mom", k) for k in range(n_mom)], 1)
        owners = (lax.axis_index("mom") - jnp.arange(n_mom)) % n_mom
        sigma = jnp.zeros_like(parts).at[:, owners].set(parts)
        packed, tile = transport(scalars, sigma, ham, hop)
        flow = tile[0, 0]
        for axis, size in (("mom", n_mom), ("energy", n_energy)):
            by = 1
            while by < size:
                flow = flow + lax.ppermute(flow, axis, [(i, i ^ by) for i in range(size)])
                by = 2 * by
        return (*spread(packed), flow)

    def keep(share, packed, flow):
        return (*spread(packed), flow.reshape(()))

    branch = missed.reshape(())
    less_new, great_new, current = lax.switch(branch, [keep, again], share, packed, flow)
    return (less_new[:, None, None], great_new[:, None, None], current)


def solution(mesh):
    return jax.shard_map(
        shards,
        mesh=mesh,
        in_specs=(
            P(None, "energy", "mom", None, None, None, None),
            P(None, "energy", "mom", None, None, None, None),
            P("mom", None, None, None, None),
            P("mom", None, None, None),
            P(),
            P(),
        ),
        out_specs=(
            P(None, "energy", "mom", None, None, None, None),
            P(None, "energy", "mom", None, None, None, None),
            P(),
        ),
        check_vma=False,
    )
```

```python
import functools

import jax
import jax.numpy as jnp
from jax import lax
from jax.experimental import pallas as pl
from jax.experimental.pallas import tpu as pltpu
from jax.sharding import PartitionSpec as P

SMAX = 7
POINTS = 128
broaden = 0.2
contact_rate = 0.5
left_level = 0.3
right_level = -0.3
thermal = 0.1
band_edge = 2.0

W = 128
BF = jnp.bfloat16
F32 = jnp.float32
LEAST = 0.03


def store(ref, real, imag):
    for row, part in ((0, real), (W, imag)):
        high = part.astype(BF)
        ref[row : row + W, :W] = high
        ref[row : row + W, W:] = (part - high.astype(F32)).astype(BF)


def store_high(ref, real, imag):
    ref[:W, :W] = real.astype(BF)
    ref[W:, :W] = imag.astype(BF)


def unpacked(value, rows, cols):
    turned = value.T
    real = jnp.where(rows < cols, value, jnp.where(rows > cols, -turned, 0.0))
    imag = jnp.where(rows >= cols, value, turned)
    return real, imag


def twofold(ref, column):
    real, imag = ref[:W, column : column + W], ref[W:, column : column + W]
    return jnp.concatenate([jnp.concatenate([real, imag], 1), jnp.concatenate([-imag, real], 1)], 0)


def product(left, right, dagger=False, high=False):
    dims = (((1,), (1,)), ((), ())) if dagger else (((1,), (0,)), ((), ()))
    top = jnp.concatenate([left[:W, :W], left[W:, :W]], 1)
    if high:
        full = lax.dot_general(top, twofold(right, 0), dims, preferred_element_type=F32)
        return full[:, :W], full[:, W:]
    bottom = jnp.concatenate([left[:W, W:], left[W:, W:]], 1)
    both = jnp.concatenate([top, bottom], 0)
    full = lax.dot_general(both, twofold(right, 0), dims, preferred_element_type=F32)
    rest = lax.dot_general(top, twofold(right, W), dims, preferred_element_type=F32)
    full = full[:W] + full[W:] + rest
    return full[:, :W], full[:, W:]


FAST_LOW = 0.006
FAST_TOP = 0.4
FAST_GROW = 5
FAST_REFINE = 2
RESIDUAL = 1.0e-4


def schedule():
    lowest, steps = FAST_LOW, []
    for step in range(FAST_GROW):
        used = max(lowest, LEAST)
        a = 4.0 / (1.0 + used)
        b = a / (1.0 + used)
        lowest = min(lowest * (a - b * lowest), b * used)
        centre = 2.0 / (1.0 + lowest) if step == FAST_GROW - 1 else 1.0
        steps.append((a * centre, b * centre))
    return steps


class Solver:
    names = (
        "hop_f", "sys_f", "inv_f", "tmp_f", "inj_f", "gr_f", "t_f", "l_f", "full_f",
        "inv", "gl", "gr", "rho",
    )

    def __init__(self, fast, sigma, scal, ham, out, scratch, base=0):
        self.fast = fast
        self.sigma = sigma
        self.scal = lambda row, e: scal[row, base + e]
        self.ham = ham
        self.out = out
        for name, ref in zip(self.names, scratch, strict=True):
            setattr(self, name, ref)
        self.count = self.inv.shape[0]
        self.weight = 2.0 * band_edge / POINTS
        self.slabs = ham.shape[0]
        self.energies = range(self.count)
        self.rows = lax.broadcasted_iota(jnp.int32, (W, W), 0)
        self.cols = lax.broadcasted_iota(jnp.int32, (W, W), 1)
        self.eye = jnp.where(self.rows == self.cols, 1.0, 0.0).astype(F32)

    @classmethod
    def scratch(cls, count, slabs):
        form = (2 * W, 2 * W)
        blocks = (count, 2, W, W)
        few = pltpu.VMEM((count,) + form, BF)
        many = pltpu.VMEM((slabs, count) + form, BF)
        every = pltpu.VMEM((slabs,) + blocks, F32)
        own = pltpu.VMEM(blocks, F32)
        return [
            pltpu.VMEM(form, BF), few, few, few, few, many, many, many,
            pltpu.VMEM((2, count) + form, BF), own, every, every, pltpu.VMEM((8, W), F32),
        ]

    def start(self, hop):
        store(self.hop_f, hop[0].T, -hop[1].T)
        self.rho[...] = jnp.zeros((8, W), F32)

    def block(self, sigma, slab, kind, e):
        return unpacked(sigma(slab, kind, e), self.rows, self.cols)

    def grow_step(self, a, b, whole):
        for e in self.energies:
            real, imag = product(self.inv_f.at[e], self.sys_f.at[e], high=True)
            store_high(self.tmp_f.at[e], real, imag)
        for e in self.energies:
            real, imag = product(self.tmp_f.at[e], self.inv_f.at[e], high=True)
            real = a * self.inv[e, 0] - b * real
            imag = a * self.inv[e, 1] - b * imag
            self.inv[e, 0] = real
            self.inv[e, 1] = imag
            (store if whole else store_high)(self.inv_f.at[e], real, imag)

    def whole_form(self):
        for e in self.energies:
            store(self.inv_f.at[e], self.inv[e, 0], self.inv[e, 1])

    def refine_step(self, slab=None):
        sizes = []
        for e in self.energies:
            real, imag = product(self.inv_f.at[e], self.sys_f.at[e])
            real = self.eye - real
            sizes.append(jnp.sum(real * real + imag * imag, axis=0, keepdims=True))
            store_high(self.tmp_f.at[e], real, -imag)
        for e in self.energies:
            real, imag = product(self.tmp_f.at[e], self.inv_f.at[e], high=True)
            real = self.inv[e, 0] + real
            imag = self.inv[e, 1] + imag
            place = (e,) if slab is None else (slab, e)
            values, form = (self.inv, self.inv_f) if slab is None else (self.gr, self.gr_f)
            values[(*place, 0)] = real
            values[(*place, 1)] = imag
            store(form.at[place], real, imag)
        return sizes

    def invert(self, slab, midway):
        norms = []
        for e in self.energies:
            real, imag = product(self.inv_f.at[e], self.sys_f.at[e], high=True)
            norms.append(jnp.sum(jnp.sqrt(real * real + imag * imag), axis=0, keepdims=True))
            if self.fast:
                store_high(self.tmp_f.at[e], real, imag)
        bound = 1.05 * jnp.max(functools.reduce(jnp.maximum, norms))
        if self.fast:
            steps = schedule()
            scale = 1.0 / (FAST_TOP * bound)
            first = steps[0][0] * scale
            second = steps[0][1] * scale * scale
            for e in self.energies:
                real, imag = product(self.tmp_f.at[e], self.inv_f.at[e], high=True)
                real = first * self.inv[e, 0] - second * real
                imag = first * self.inv[e, 1] - second * imag
                self.inv[e, 0] = real
                self.inv[e, 1] = imag
                store_high(self.inv_f.at[e], real, imag)
            for place, (a, b) in enumerate(steps[1:]):
                self.grow_step(a, b, place == FAST_GROW - 2)
                if place == 1 and midway is not None:
                    midway()
            for step in range(FAST_REFINE):
                sizes = self.refine_step(slab if step == FAST_REFINE - 1 else None)
            self.rho[0:1] = self.rho[0:1] + functools.reduce(jnp.add, sizes)
            return
        scale = 1.0 / bound
        for e in self.energies:
            real = self.inv[e, 0] * scale
            imag = self.inv[e, 1] * scale
            self.inv[e, 0] = real
            self.inv[e, 1] = imag
        self.whole_form()

        def grow(carry):
            lowest, done = carry
            used = jnp.maximum(lowest, LEAST)
            a = 4.0 / (1.0 + used)
            b = a / (1.0 + used)
            after = jnp.minimum(lowest * (a - b * lowest), b * used)
            for e in self.energies:
                real, imag = product(self.inv_f.at[e], self.sys_f.at[e])
                store(self.tmp_f.at[e], real, imag)
            for e in self.energies:
                real, imag = product(self.tmp_f.at[e], self.inv_f.at[e])
                real = a * self.inv[e, 0] - b * real
                imag = a * self.inv[e, 1] - b * imag
                self.inv[e, 0] = real
                self.inv[e, 1] = imag
                store(self.inv_f.at[e], real, imag)
            return after, done + 1

        lax.while_loop(
            lambda carry: jnp.logical_and(carry[0] < 0.9, carry[1] < 64),
            grow,
            (broaden * broaden * scale, jnp.int32(0)),
        )

        def refine(carry):
            sizes = [jnp.sum(size) for size in self.refine_step()]
            return functools.reduce(jnp.maximum, sizes), carry[1] + 1

        lax.while_loop(
            lambda carry: jnp.logical_and(carry[0] > 4.0e-6, carry[1] < 24),
            refine,
            (jnp.float32(1.0), jnp.int32(0)),
        )

    def level(self, slab, last, midway=None, sigma=None):
        sigma = self.sigma if sigma is None else sigma
        at_left = 0.0 if last else jnp.where(slab == 0, 1.0, 0.0)
        for e in self.energies:
            less = self.block(sigma, slab, 0, e)
            great = self.block(sigma, slab, 1, e)
            fill = self.scal(2, e) if last else at_left * self.scal(1, e)
            contact = contact_rate if last else at_left * contact_rate
            sys_r = self.scal(0, e) * self.eye - self.ham[slab, 0] - 0.5 * (great[0] - less[0])
            sys_i = (broaden + contact) * self.eye - self.ham[slab, 1] - 0.5 * (great[1] - less[1])
            inj_r = less[0]
            inj_i = less[1] + 2.0 * contact_rate * fill * self.eye
            if not last:
                real, imag = product(self.t_f.at[slab + 1, e], self.hop_f, dagger=True)
                sys_r = sys_r - real
                sys_i = sys_i - imag
                real, imag = product(self.l_f.at[slab + 1, e], self.hop_f, dagger=True)
                inj_r = inj_r + real
                inj_i = inj_i + imag
            store(self.sys_f.at[e], sys_r, sys_i)
            store(self.inj_f.at[e], inj_r, inj_i)
            back_r = sys_r.T
            back_i = -sys_i.T
            self.inv[e, 0] = back_r
            self.inv[e, 1] = back_i
            store_high(self.inv_f.at[e], back_r, back_i)
        self.invert(slab, midway)
        for e in self.energies:
            if not self.fast:
                self.gr[slab, e] = self.inv[e]
                self.gr_f[slab, e] = self.inv_f[e]
            real, imag = product(self.gr_f.at[slab, e], self.inj_f.at[e])
            store(self.tmp_f.at[e], real, imag)
        for e in self.energies:
            real, imag = product(self.tmp_f.at[e], self.gr_f.at[slab, e], dagger=True)
            self.gl[slab, e, 0] = real
            self.gl[slab, e, 1] = imag
            store(self.inj_f.at[e], real, imag)

    def fold(self, slab):
        for e in self.energies:
            real, imag = product(self.hop_f, self.gr_f.at[slab, e])
            store(self.t_f.at[slab, e], real, imag)
            real, imag = product(self.hop_f, self.inj_f.at[e])
            store(self.l_f.at[slab, e], real, imag)

    def flow(self):
        flow = jnp.zeros((1, W), F32)
        for e in self.energies:
            fill = self.scal(1, e)
            less = self.gl[0, e, 1]
            mixed = fill * (less + 2.0 * self.gr[0, e, 1]) + (1.0 - fill) * less
            flow = flow - jnp.sum(mixed * self.eye, axis=0, keepdims=True)
        flow = jnp.broadcast_to(jnp.sum(flow, axis=1, keepdims=True) * self.weight, (8, W))
        missed = jnp.broadcast_to(jnp.sum(self.rho[0:1], axis=1, keepdims=True), (8, W))
        missed = jnp.where(missed <= RESIDUAL, 0.0, 1.0)
        return jnp.where(lax.broadcasted_iota(jnp.int32, (8, W), 0) == 0, flow, missed)

    def finish(self, slab, e, green, less):
        great = (less[0] + green[0] - green[0].T, less[1] + green[1] + green[1].T)
        upper = self.rows < self.cols
        self.out[e, slab, 0] = jnp.where(upper, less[0], less[1])
        self.out[e, slab, 1] = jnp.where(upper, great[0], great[1])
        store(self.full_f.at[0, e], *green)
        store(self.full_f.at[1, e], *less)

    def first(self):
        for e in self.energies:
            self.finish(0, e, (self.gr[0, e, 0], self.gr[0, e, 1]), (self.gl[0, e, 0], self.gl[0, e, 1]))

    def up(self, slab):
        for e in self.energies:
            real, imag = product(self.gr_f.at[slab, e], self.hop_f, dagger=True)
            store(self.sys_f.at[e], real, imag)
        for e in self.energies:
            real, imag = product(self.sys_f.at[e], self.full_f.at[0, e])
            store(self.tmp_f.at[e], real, imag)
            real, imag = product(self.sys_f.at[e], self.full_f.at[1, e])
            store(self.inj_f.at[e], real, imag)
        for e in self.energies:
            real, imag = product(self.tmp_f.at[e], self.t_f.at[slab, e])
            green = (self.gr[slab, e, 0] + real, self.gr[slab, e, 1] + imag)
            cross = product(self.tmp_f.at[e], self.l_f.at[slab, e])
            real, imag = product(self.inj_f.at[e], self.sys_f.at[e], dagger=True)
            less = (
                self.gl[slab, e, 0] + real + cross[0] - cross[0].T,
                self.gl[slab, e, 1] + imag + cross[1] + cross[1].T,
            )
            self.finish(slab, e, green, less)


def rows_of(sigma_ref):
    def read(slab, kind, e):
        return jnp.concatenate([sigma_ref[slab, owner, kind, e] for owner in range(sigma_ref.shape[1])], 0)

    return read


def sure_kernel(fast, scal_ref, sig_ref, ham_ref, hop_ref, out_ref, flow_ref, *scratch):
    base = pl.program_id(0) * sig_ref.shape[3]
    solver = Solver(fast, rows_of(sig_ref), scal_ref, ham_ref, out_ref, scratch, base)
    slabs = solver.slabs
    solver.start(hop_ref)
    solver.level(slabs - 1, True)

    def down(step, carry):
        slab = slabs - 2 - step
        solver.fold(slab + 1)
        solver.level(slab, False)
        return carry

    lax.fori_loop(0, slabs - 1, down, 0)
    flow_ref[0] = solver.flow()
    solver.first()

    def up(slab, carry):
        solver.up(slab)
        return carry

    lax.fori_loop(1, slabs, up, 0)


def transport(scalars, sigma, hamiltonian, coupling, fast=False):
    slabs, owners, _, count, depth = sigma.shape[:5]
    some = count if fast else 1
    vmem = pl.BlockSpec(memory_space=pltpu.VMEM)
    blocks = jax.ShapeDtypeStruct((count, slabs, 2, W, W), F32)
    out_spec = pl.BlockSpec((some, slabs, 2, W, W), lambda e: (e, 0, 0, 0, 0))
    packed, flow = pl.pallas_call(
        functools.partial(sure_kernel, fast),
        grid=(count // some,),
        out_shape=(blocks, jax.ShapeDtypeStruct((count // some, 8, W), F32)),
        in_specs=[
            pl.BlockSpec(memory_space=pltpu.SMEM),
            pl.BlockSpec((slabs, owners, 2, some, depth, W), lambda e: (0, 0, 0, e, 0, 0)),
            vmem,
            vmem,
        ],
        out_specs=(out_spec, pl.BlockSpec((1, 8, W), lambda e: (e, 0, 0))),
        scratch_shapes=Solver.scratch(some, slabs),
        compiler_params=pltpu.CompilerParams(vmem_limit_bytes=(44 if fast else 16) * 1024 * 1024),
        cost_estimate=pl.CostEstimate(flops=20_000_000_000, bytes_accessed=8_000_000, transcendentals=0),
    )(scalars, sigma, hamiltonian, coupling)
    return packed, jnp.sum(flow, axis=0)


def spread_kernel(packed_ref, less_ref, great_ref):
    rows = lax.broadcasted_iota(jnp.int32, (W, W), 0)
    cols = lax.broadcasted_iota(jnp.int32, (W, W), 1)
    for slab in range(packed_ref.shape[1]):
        for kind, ref in enumerate((less_ref, great_ref)):
            real, imag = unpacked(packed_ref[0, slab, kind], rows, cols)
            ref[0, slab, 0] = real
            ref[0, slab, 1] = imag


def spread(packed):
    spec = pl.BlockSpec((1,) + packed.shape[1:], lambda e: (e, 0, 0, 0, 0))
    return pl.pallas_call(
        spread_kernel,
        grid=(packed.shape[0],),
        out_shape=(jax.ShapeDtypeStruct(packed.shape, F32),) * 2,
        in_specs=[spec],
        out_specs=(spec, spec),
        compiler_params=pltpu.CompilerParams(vmem_limit_bytes=16 * 1024 * 1024),
    )(packed)


MESH = pl.DeviceIdType.MESH
GATHERED = 2


def remote(source, target, send_sem, recv_sem, peer):
    return pltpu.make_async_remote_copy(
        src_ref=source, dst_ref=target, send_sem=send_sem, recv_sem=recv_sem,
        device_id=peer, device_id_type=MESH,
    )


def exchange_kernel(
    by, n_energy, n_mom,
    weight_ref, less_hbm, great_hbm, sigma_ref,
    less_ref, great_ref, load_sem, pack, near_a, near_b, half_a, half_b, share, high, low, send_sem, recv_sem,
):
    place = lax.axis_index("energy")
    me = lax.axis_index("mom")
    slabs, count = less_ref.shape[:2]
    depth = W // n_mom
    loads = [
        [
            pltpu.make_async_copy(source.at[:, c], target.at[c], load_sem.at[kind, c])
            for kind, (source, target) in enumerate(((less_hbm, less_ref), (great_hbm, great_ref)))
        ]
        for c in range(slabs)
    ]
    for c in range(slabs - 1, -1, -1):
        for load in loads[c]:
            load.start()
    after = lax.rem(me + 1, n_mom)
    before = lax.rem(me + n_mom - 1, n_mom)
    across = lax.rem(me + 2, n_mom)
    over = {"energy": lax.rem(place + by, n_energy)}
    under = {"energy": lax.rem(place - by + n_energy, n_energy)}
    wrapped_up = lax.div(place + by, n_energy)
    wrapped_down = 1 - lax.div(place - by + n_energy, n_energy)
    kept_up = (1 - wrapped_up).astype(F32)
    kept_down = (1 - wrapped_down).astype(F32)
    emission = weight_ref[0] * (1.0 / n_mom)
    absorption = weight_ref[1] * (1.0 / n_mom)

    barrier = pltpu.get_barrier_semaphore()
    for peer in ({"mom": after}, {"mom": before}, over, under):
        pl.semaphore_signal(barrier, inc=1, device_id=peer, device_id_type=MESH)

    def send(kind, chunk, source, target, peer):
        copy = remote(source, target, send_sem.at[kind, chunk], recv_sem.at[kind, chunk], peer)
        copy.start()
        return copy

    sent = {}

    def pass_on(c):
        sent[6, c].wait_recv()
        part = sigma_ref.at[c, before, 0]
        sent[8, c] = send(8, c, part, part, {"mom": after})
        sent[7, c].wait_recv()
        part = sigma_ref.at[c, after, 1]
        sent[9, c] = send(9, c, part, part, {"mom": before})

    rows = lax.broadcasted_iota(jnp.int32, (depth, W), 0)
    cols = lax.broadcasted_iota(jnp.int32, (depth, W), 1)
    order = range(slabs - 1, -1, -1)
    for c in order:
        for load in loads[c]:
            load.wait()
        for part in range(n_mom):
            span = slice(part * depth, (part + 1) * depth)
            upper = cols > rows + part * depth
            for kind, ref in enumerate((less_ref, great_ref)):
                pack[c, part, kind] = jnp.where(upper, ref[c, :, 0, span], ref[c, :, 1, span])
        if c == slabs - 1:
            pl.semaphore_wait(barrier, 4)
        sent[0, c] = send(0, c, pack.at[c, across, 0], near_a.at[c], {"mom": after})
        sent[1, c] = send(1, c, pack.at[c, across, 1], near_b.at[c], {"mom": before})
    for c in order:
        sent[0, c].wait_recv()
        pack[c, after, 0] = pack[c, after, 0] + near_a[c]
        sent[1, c].wait_recv()
        pack[c, before, 1] = pack[c, before, 1] + near_b[c]
        sent[2, c] = send(2, c, pack.at[c, after], half_a.at[c], {"mom": after})
        sent[3, c] = send(3, c, pack.at[c, before], half_b.at[c], {"mom": before})
    def settle(c):
        sent[2, c].wait_recv()
        sent[3, c].wait_recv()
        share[c] = pack[c, me] + (half_a[c] + half_b[c])
        sent[4, c] = send(4, c, share.at[c], high.at[c], under)
        sent[5, c] = send(5, c, share.at[c], low.at[c], over)
    def combine(c):
        sent[4, c].wait_recv()
        sent[5, c].wait_recv()
        for j in range(count):
            if j < count - 1:
                up = [high[c, kind, j + wrapped_up] for kind in range(2)]
            else:
                up = [high[c, kind, j] * kept_up for kind in range(2)]
            if j > 0:
                down = [low[c, kind, j - wrapped_down] for kind in range(2)]
            else:
                down = [low[c, kind, j] * kept_down for kind in range(2)]
            sigma_ref[c, me, 0, j] = emission * up[0] + absorption * down[0]
            sigma_ref[c, me, 1, j] = emission * down[1] + absorption * up[1]
        if c >= slabs - GATHERED:
            mine = sigma_ref.at[c, me]
            sent[6, c] = send(6, c, mine, mine, {"mom": after})
            sent[7, c] = send(7, c, mine, mine, {"mom": before})

    last = slabs - 1
    settle(last)
    for c in range(last - 1, -1, -1):
        settle(c)
        combine(c + 1)
    pass_on(last)
    combine(0)
    for kind, c in ((8, last), (9, last), *((kind, c) for c in range(slabs - GATHERED, last) for kind in (6, 7))):
        sent[kind, c].wait_recv()
    for copy in sent.values():
        copy.wait_send()


def exchange(by, n_energy, n_mom, weight, lesser, greater):
    count, slabs = lesser.shape[:2]
    depth = W // n_mom
    vmem = pl.BlockSpec(memory_space=pltpu.VMEM)
    hbm = pl.BlockSpec(memory_space=pl.ANY)
    block = pltpu.VMEM((slabs, count, 2, W, W), F32)
    half = pltpu.VMEM((slabs, count, depth, W), F32)
    whole = pltpu.VMEM((slabs, 2, count, depth, W), F32)
    return pl.pallas_call(
        functools.partial(exchange_kernel, by, n_energy, n_mom),
        out_shape=jax.ShapeDtypeStruct((slabs, n_mom, 2, count, depth, W), F32),
        in_specs=[pl.BlockSpec(memory_space=pltpu.SMEM), hbm, hbm],
        out_specs=vmem,
        scratch_shapes=[
            block, block, pltpu.SemaphoreType.DMA((2, slabs)),
            pltpu.VMEM((slabs, n_mom, 2, count, depth, W), F32),
            half, half, whole, whole, whole, whole, whole,
            pltpu.SemaphoreType.DMA((10, slabs)),
            pltpu.SemaphoreType.DMA((10, slabs)),
        ],
        compiler_params=pltpu.CompilerParams(
            collective_id=by, has_side_effects=True, vmem_limit_bytes=32 * 1024 * 1024
        ),
    )(weight, lesser, greater)


def fast_kernel(
    n_mom, inner, outer,
    scal_ref, share_ref, ham_ref, hop_ref, out_ref, flow_ref, missed_ref,
    sigma, first, second, tile, partial, send_sem, recv_sem, sum_send, sum_recv, *scratch,
):
    solver = Solver(True, rows_of(sigma), scal_ref, ham_ref, out_ref, scratch)
    slabs = solver.slabs
    place = lax.axis_index("energy")
    me = lax.axis_index("mom")
    after = lax.rem(me + 1, n_mom)
    before = lax.rem(me + n_mom - 1, n_mom)
    low = lax.rem(place, inner)
    high = lax.div(place, inner)
    slot = high * n_mom + me

    def outer_peer(step):
        other = lax.rem(slot + step, outer)
        return other, {"energy": lax.div(other, n_mom) * inner + low, "mom": lax.rem(other, n_mom)}

    def inner_peer(step):
        other = lax.rem(low + step, inner)
        return other, {"energy": high * inner + other, "mom": me}

    barrier = pltpu.get_barrier_semaphore()
    for step in range(1, outer):
        pl.semaphore_signal(barrier, inc=1, device_id=outer_peer(step)[1], device_id_type=MESH)
    for step in range(1, inner):
        pl.semaphore_signal(barrier, inc=1, device_id=inner_peer(step)[1], device_id_type=MESH)

    def near(slab):
        for kind, peer in ((0, after), (1, before)):
            yield remote(
                share_ref.at[slab, me], sigma.at[slab, me],
                send_sem.at[kind, slab], recv_sem.at[kind, slab], {"mom": peer},
            )

    def far(slab, source=sigma):
        for kind, owner, peer in ((0, before, after), (1, after, before)):
            yield remote(
                source.at[slab, owner, kind], sigma.at[slab, owner, kind], send_sem.at[2 + kind, slab], recv_sem.at[2 + kind, slab], {"mom": peer}
            )

    def started(copies):
        for copy in copies:
            copy.start()

    def arrived(copies):
        for copy in copies:
            copy.wait_recv()

    rest = range(slabs - GATHERED - 1, -1, -1)
    nearly = range(slabs - GATHERED, slabs - 1)

    def share_rest():
        pl.semaphore_wait(barrier, outer + inner - 2)
        for slab in nearly:
            started(far(slab, share_ref))
            for owner in (me, before, after):
                sigma[slab, owner] = share_ref[slab, owner]
        for slab in rest:
            started(near(slab))
            sigma[slab, me] = share_ref[slab, me]

    solver.start(hop_ref)
    solver.level(slabs - 1, True, share_rest, rows_of(share_ref))

    def down(step, carry):
        slab = slabs - 2 - step

        def pass_on(others):
            @pl.when(step == 0)
            def _():
                for other in others:
                    arrived(near(other))
                    started(far(other))

        solver.fold(slab + 1)
        pass_on(rest[:1])
        arrived(far(slab))
        solver.level(slab, False, lambda: pass_on(rest[1:]))
        return carry

    lax.fori_loop(0, slabs - 1, down, 0)

    def round_of(source, slots, size, own, peer, base):
        def copy(index, step):
            return remote(
                source, slots.at[index], sum_send.at[base + step], sum_recv.at[base + index], peer(step)[1]
            )

        def begin():
            for step in range(1, size):
                copy(own, step).start()
            slots[own] = source[...]

        def end():
            for step in range(1, size):
                copy(peer(step)[0], step).wait_recv()
            result = slots[0]
            for index in range(1, size):
                result = result + slots[index]
            for step in range(1, size):
                copy(own, step).wait_send()
            return result

        return begin, end

    begin_outer, end_outer = round_of(tile, first, outer, slot, outer_peer, 0)
    begin_inner, end_inner = round_of(partial, second, inner, low, inner_peer, outer)
    tile[...] = solver.flow()
    solver.first()
    begin_outer()
    for slab in range(1, slabs - 1):
        solver.up(slab)
    partial[...] = end_outer()
    begin_inner()
    solver.up(slabs - 1)
    total = end_inner()
    flow_ref[...] = total[0:1, 0:1]
    missed_ref[...] = jnp.where(total[1:2, 0:1] > 0.5, 1, 0)
    for slab in rest:
        for copy in near(slab):
            copy.wait_send()
    for slab in (*nearly, *rest):
        for copy in far(slab):
            copy.wait_send()


def quick(n_energy, n_mom, scalars, share, hamiltonian, coupling, inner=8):
    slabs, _, _, count, depth = share.shape[:5]
    outer = n_energy // inner * n_mom
    vmem = pl.BlockSpec(memory_space=pltpu.VMEM)
    blocks = jax.ShapeDtypeStruct((count, slabs, 2, W, W), F32)
    return pl.pallas_call(
        functools.partial(fast_kernel, n_mom, inner, outer),
        out_shape=(
            blocks,
            jax.ShapeDtypeStruct((1, 1), F32),
            jax.ShapeDtypeStruct((1, 1), jnp.int32),
        ),
        in_specs=[pl.BlockSpec(memory_space=pltpu.SMEM), vmem, vmem, vmem],
        out_specs=(vmem, vmem, vmem),
        scratch_shapes=[
            pltpu.VMEM((slabs, n_mom, 2, count, depth, W), F32),
            pltpu.VMEM((outer, 8, W), F32),
            pltpu.VMEM((inner, 8, W), F32),
            pltpu.VMEM((8, W), F32),
            pltpu.VMEM((8, W), F32),
            pltpu.SemaphoreType.DMA((4, slabs)),
            pltpu.SemaphoreType.DMA((4, slabs)),
            pltpu.SemaphoreType.DMA((outer + inner,)),
            pltpu.SemaphoreType.DMA((outer + inner,)),
        ]
        + Solver.scratch(count, slabs),
        compiler_params=pltpu.CompilerParams(
            collective_id=SMAX + 1, has_side_effects=True, vmem_limit_bytes=26 * 1024 * 1024
        ),
    )(scalars, share, hamiltonian, coupling)


def moved(array, axis, by):
    size = lax.axis_size(axis)
    return lax.ppermute(array, axis, [(i, (i + by) % size) for i in range(size)]) if by else array


def shards(lesser, greater, hamiltonian, coupling, shift, phonon_weight):
    n_energy = lax.axis_size("energy")
    n_mom = lax.axis_size("mom")
    here = lax.axis_index("energy")
    count = lesser.shape[0]
    total = count * n_energy
    branches = [functools.partial(exchange, k + 1, n_energy, n_mom) for k in range(SMAX)]
    share = lax.switch(shift[0] - 1, branches, phonon_weight, lesser[:, 0, 0], greater[:, 0, 0])
    grid = (jnp.arange(count) * n_energy + here).astype(F32)
    energy = (grid + 0.5) * (2.0 * band_edge / total) - band_edge
    scalars = jnp.stack(
        [
            energy,
            jax.nn.sigmoid((left_level - energy) / thermal),
            jax.nn.sigmoid((right_level - energy) / thermal),
        ]
    )
    ham, hop = hamiltonian[0], coupling[0]
    packed, flow, missed = quick(n_energy, n_mom, scalars, share, ham, hop)

    def again(share, packed, flow):
        mine = share[:, lax.axis_index("mom")]
        parts = jnp.stack([moved(mine, "mom", k) for k in range(n_mom)], 1)
        owners = (lax.axis_index("mom") - jnp.arange(n_mom)) % n_mom
        sigma = jnp.zeros_like(parts).at[:, owners].set(parts)
        packed, tile = transport(scalars, sigma, ham, hop)
        flow = tile[0, 0]
        for axis, size in (("mom", n_mom), ("energy", n_energy)):
            by = 1
            while by < size:
                flow = flow + lax.ppermute(flow, axis, [(i, i ^ by) for i in range(size)])
                by = 2 * by
        return (*spread(packed), flow)

    def keep(share, packed, flow):
        return (*spread(packed), flow.reshape(()))

    branch = missed.reshape(())
    less_new, great_new, current = lax.switch(branch, [keep, again], share, packed, flow)
    return (less_new[:, None, None], great_new[:, None, None], current)


def solution(mesh):
    return jax.shard_map(
        shards,
        mesh=mesh,
        in_specs=(
            P(None, "energy", "mom", None, None, None, None),
            P(None, "energy", "mom", None, None, None, None),
            P("mom", None, None, None, None),
            P("mom", None, None, None),
            P(),
            P(),
        ),
        out_specs=(
            P(None, "energy", "mom", None, None, None, None),
            P(None, "energy", "mom", None, None, None, None),
            P(),
        ),
        check_vma=False,
    )
```
